768 devices in a mesh: tile: 16 (over z_hi, y), col: 48 (over x, z_lo, core).
Axes of the slice: x: 4, y: 8, z: 12 (z_hi: 2, z_lo: 6; z = z_hi * 6 + z_lo), core: 2. Of those that a mesh axis runs over, the one named last changes fastest.
Arguments:
- adjoint_in: float32 [25, 512, 6144], P(None, 'tile', 'col'), may hold values from -6 to 6
- centre: float32 [25, 512, 6144], P(None, 'tile', 'col'), may hold values from 0.2 to 0.6
- side_coeff: float32 [4, 25, 512, 6144], P(None, None, 'tile', 'col'), may hold values from 0.05 to 0.25
- vert_coeff: float32 [2, 25, 512, 6144], P(None, None, 'tile', 'col'), may hold values from 0.05 to 0.25
- land_mask: int32 [25, 512, 6144], P(None, 'tile', 'col'), may hold values 0 or 1
- obs_misfit: float32 [16, 48, 48, 128], P('tile', 'col'), may hold values from -6 to 6
- obs_cell: int32 [16, 48, 48, 128], P('tile', 'col'), may hold values from 0 to 102399
- obs_count: int32 [16, 48, 48], P('tile', 'col'), may hold values from 0 to 128, as said below
- fold_partner: int32 [48], replicated, may hold values from 0 to 47, as said below
- fold_flip: int32 [48], replicated, may hold values 0 or 1
Outputs:
- adjoint_out: float32 [25, 512, 6144], P(None, 'tile', 'col')
The draws below stay inside these ranges and needn't reach their ends.
Inputs may be any that keep to these rules, and one draw needn't show every extreme that they name: `obs_count`: slots at and beyond the count hold values that are ignored; some destination gets 128 from some source in every draw. `fold_partner`: each tile column appears exactly once.
All inputs are finite; a program needn't handle non-finite values. No bound on the sum of `land_mask` on one device may be relied on, other than what follows from the above.
Results may differ from the reference program's by a relative error of at most 0.0003.
Values sent between devices are 32-bit elements; how exact they have to be, the bound alone decides.
A program may use at most 64 MiB of HBM per device.

```python
import jax
import jax.numpy as jnp

LEVELS = 25
ROWS = 32
COLS = 128
CAP = 128
STEPS = 2
TILE_ROWS = 16
TILE_COLS = 48
NY = 512
NX = 6144


def draw_obs_count(key, part):
    key_base, key_dense, key_full, key_empty = jax.random.split(key, 4)
    base = jax.random.randint(key_base, (TILE_ROWS, TILE_COLS, TILE_COLS), 0, CAP + 1)
    dense = jax.random.randint(key_dense, (1, TILE_COLS, 1), 1, 4)
    counts = jnp.minimum(CAP, base * dense // 2)
    empty_at = jax.random.randint(key_empty, (3,), 0, 1000000)
    full_at = jax.random.randint(key_full, (3,), 0, 1000000)
    counts = counts.at[empty_at[0] % TILE_ROWS, empty_at[1] % TILE_COLS, empty_at[2] % TILE_COLS].set(0)
    counts = counts.at[full_at[0] % TILE_ROWS, full_at[1] % TILE_COLS, full_at[2] % TILE_COLS].set(CAP)
    return counts.astype(jnp.int32)


def place_value(order, position, wanted):
    spots = jnp.arange(TILE_COLS, dtype=jnp.int32)
    found = jnp.sum(jnp.where(order == wanted, spots, 0)).astype(jnp.int32)
    moved = order[position]
    order = jnp.where(spots == found, moved, order)
    order = jnp.where(spots == position, wanted, order)
    return order


def draw_fold_partner(key, part):
    order = jax.random.permutation(jax.random.fold_in(key, 7), TILE_COLS).astype(jnp.int32)
    order = place_value(order, 0, 1 % TILE_COLS)
    order = place_value(order, 1, (1 + TILE_COLS // 2) % TILE_COLS)
    return order.astype(jnp.int32)


def with_ends(drawn, stream_key, least, top_value):
    longest = drawn.shape.index(max(drawn.shape))
    spots = []
    for shift in (0, 1):
        where = [jax.random.randint(jax.random.fold_in(stream_key, axis), (), 0, length) for axis, length in enumerate(drawn.shape)]
        where[longest] = (where[longest] + shift) % drawn.shape[longest]
        spots.append(tuple(where))
    return drawn.at[spots[0]].set(least).at[spots[1]].set(top_value)


def steps_of(key, dims, cuts, low, high):
    loudness, own = 1.0, jax.random.fold_in(key, 6)
    for dim, blocks in cuts:
        heights = jnp.exp(jax.random.uniform(jax.random.fold_in(own, dim), (blocks,), jnp.float32, low / len(cuts), high / len(cuts)))
        loudness = loudness * jnp.repeat(heights, dims[dim] // blocks).reshape([-1 if axis == dim else 1 for axis in range(len(dims))])
    return loudness


def scatter_about(stream_key, extent, scale, limit, cuts=(), held_as=jnp.bfloat16):
    entries = scale * jax.random.normal(stream_key, extent, jnp.float32)
    if cuts:
        entries = entries * steps_of(stream_key, extent, cuts, -0.22, 0.18)
    return jnp.clip(entries, -limit, limit).astype(held_as)


def setup_inputs(seed: int = 0) -> dict:
    keys = jax.random.split(jax.random.key(seed), 11)
    return {
        "adjoint_in": scatter_about(keys[0], (LEVELS, NY, NX), 1.0, 6.0, ((1, 16), (2, 48)), jnp.float32),
        "centre": jnp.clip(0.2 + 0.400000021 * jax.random.uniform(keys[1], (LEVELS, NY, NX), jnp.float32) ** steps_of(keys[1], (LEVELS, NY, NX), ((1, 16), (2, 48)), -0.2, 0.2), 0.2, 0.6),
        "side_coeff": jnp.clip(0.05 + 0.2 * jax.random.uniform(keys[2], (4, LEVELS, NY, NX), jnp.float32) ** steps_of(keys[2], (4, LEVELS, NY, NX), ((2, 16), (3, 48)), -0.2, 0.2), 0.05, 0.25),
        "vert_coeff": jnp.clip(0.05 + 0.2 * jax.random.uniform(keys[3], (2, LEVELS, NY, NX), jnp.float32) ** steps_of(keys[3], (2, LEVELS, NY, NX), ((2, 16), (3, 48)), -0.2, 0.2), 0.05, 0.25),
        "land_mask": with_ends((jax.random.randint(keys[4], (LEVELS, NY, NX), 0, 4) < 3).astype(jnp.int32), jax.random.fold_in(keys[4], 1), 0, 1),
        "obs_misfit": scatter_about(keys[5], (TILE_ROWS, TILE_COLS, TILE_COLS, CAP), 1.0, 6.0, ((0, 16), (1, 48)), jnp.float32),
        "obs_cell": with_ends(jax.random.randint(keys[6], (TILE_ROWS, TILE_COLS, TILE_COLS, CAP), 0, LEVELS * ROWS * COLS), jax.random.fold_in(keys[6], 1), 0, (LEVELS * ROWS * COLS) - 1).astype(jnp.int32),
        "obs_count": draw_obs_count(jax.random.fold_in(keys[10], 71), 0),
        "fold_partner": draw_fold_partner(jax.random.fold_in(keys[10], 71), 0),
        "fold_flip": with_ends((jax.random.randint(keys[9], (TILE_COLS,), 0, 2) < 1).astype(jnp.int32), jax.random.fold_in(keys[9], 1), 0, 1),
    }


def tile_forcing(misfit, cells, counts):
    usable = jnp.arange(misfit.shape[1])[None, :] < counts[:, None]
    values = jnp.where(usable, misfit, jnp.float32(0.0))
    total = jnp.zeros((LEVELS * ROWS * COLS,), jnp.float32)
    return total.at[cells.reshape(-1)].add(values.reshape(-1))


def adjoint_step(adjoint, centre, side_coeff, vert_coeff, fold_partner, fold_flip, ocean):
    partial_value = side_coeff * adjoint[None]
    result = centre * adjoint
    result = result + jnp.roll(partial_value[0], 1, axis=2) + jnp.roll(partial_value[1], -1, axis=2)
    result = result + jnp.pad(partial_value[2], ((0, 0), (1, 0), (0, 0)))[:, :-1, :]
    result = result + jnp.pad(partial_value[3], ((0, 0), (0, 1), (0, 0)))[:, 1:, :]
    upward = vert_coeff[0] * adjoint
    downward = vert_coeff[1] * adjoint
    result = result + jnp.pad(upward, ((0, 1), (0, 0), (0, 0)))[1:]
    result = result + jnp.pad(downward, ((1, 0), (0, 0), (0, 0)))[:-1]
    top_edge = partial_value[2][:, -1, :].reshape(LEVELS, TILE_COLS, COLS)
    turned = jnp.where(fold_flip[None, :, None] == 1, top_edge[:, :, ::-1], top_edge)
    landing = jnp.zeros_like(turned).at[:, fold_partner, :].set(turned)
    result = result.at[:, -1, :].add(landing.reshape(LEVELS, TILE_COLS * COLS))
    return ocean * result


def reference(adjoint_in, centre, side_coeff, vert_coeff, land_mask, obs_misfit, obs_cell, obs_count, fold_partner, fold_flip):
    by_landing = jnp.transpose(obs_misfit, (0, 2, 1, 3))
    forcing = jax.vmap(jax.vmap(tile_forcing))(by_landing, obs_cell, obs_count)
    forcing = forcing.reshape(TILE_ROWS, TILE_COLS, LEVELS, ROWS, COLS)
    forcing = jnp.transpose(forcing, (2, 0, 3, 1, 4)).reshape(LEVELS, TILE_ROWS * ROWS, TILE_COLS * COLS)
    adjoint = adjoint_in + forcing
    ocean = land_mask.astype(jnp.float32)
    for advance in range(STEPS):
        adjoint = adjoint_step(adjoint, centre, side_coeff, vert_coeff, fold_partner, fold_flip, ocean)
    return adjoint
```

```python
import functools

import jax
import jax.numpy as jnp
from jax import lax
from jax.experimental import pallas as pl
from jax.experimental.pallas import tpu as pltpu
from jax.sharding import PartitionSpec as P

LEVELS = 25
ROWS = 32
COLS = 128
STEPS = 2
CELL_ROWS = LEVELS * ROWS
VREGS = CELL_ROWS // 8
CHUNK = 8
MESH = pl.DeviceIdType.MESH


def grid_of(n_col):
    return (4, 6, 2) if n_col == 48 else (2, n_col // 4, 2)


def kernel(
    n_tile,
    n_col,
    adj_h,
    cen_h,
    side_h,
    vert_h,
    mask_h,
    mis_h,
    cell_h,
    cnt_s,
    fp_s,
    ff_s,
    out_ref,
    adj,
    cen,
    side,
    vert,
    mask,
    cell,
    mis,
    rows_1h,
    vals_1h,
    acc,
    y_ref,
    r_ref,
    edge_out,
    edge_in,
    col_out,
    col_in,
    line_bufs,
    pick_buf,
    group_bufs,
    load_sem,
    a2a_send,
    a2a_recv,
    edge_send,
    edge_recv,
    col_send,
    col_recv,
    line_send,
    line_recv,
    pick_send,
    pick_recv,
):
    nx, nz, nc = grid_of(n_col)
    ng = nx * nc
    me = lax.axis_index("col")
    t = lax.axis_index("tile")
    at_top = t == n_tile - 1
    core = me % nc
    my_z = (me // nc) % nz
    my_x = me // (nc * nz)
    my_g = my_x * nc + core
    east = (me + 1) % n_col
    west = (me + n_col - 1) % n_col

    loads = [
        pltpu.make_async_copy(src, dst, load_sem.at[i])
        for i, (src, dst) in enumerate(
            [
                (cell_h, cell),
                (adj_h, adj),
                (side_h, side),
                (cen_h, cen),
                (vert_h, vert),
                (mask_h, mask),
                (mis_h.at[me], mis.at[me]),
            ]
        )
    ]
    for load in loads:
        load.start()

    barrier = pltpu.get_barrier_semaphore()

    @pl.loop(1, n_col)
    def _(i):
        pl.semaphore_signal(
            barrier, inc=1, device_id={"col": (me + i) % n_col}, device_id_type=MESH
        )

    @pl.when(t > 0)
    def _():
        pl.semaphore_signal(barrier, inc=1, device_id={"tile": t - 1}, device_id_type=MESH)

    @pl.when(t < n_tile - 1)
    def _():
        pl.semaphore_signal(barrier, inc=1, device_id={"tile": t + 1}, device_id_type=MESH)

    pl.semaphore_wait(
        barrier, n_col - 1 + jnp.where(t > 0, 1, 0) + jnp.where(t < n_tile - 1, 1, 0)
    )

    @pl.loop(1, n_col)
    def _(i):
        peer = (me + i) % n_col
        pltpu.make_async_remote_copy(
            src_ref=mis_h.at[peer],
            dst_ref=mis.at[me],
            send_sem=a2a_send,
            recv_sem=a2a_recv,
            device_id={"col": peer},
            device_id_type=MESH,
        ).start()

    def find(s, found):
        target = fp_s[s]
        return tuple(
            jnp.where(target == (g // nc) * nc * nz + my_z * nc + g % nc, s, found[g])
            for g in range(ng)
        ) + (jnp.where(target == me, s, found[ng]),)

    sources = lax.fori_loop(0, n_col, find, (jnp.int32(0),) * (ng + 1))
    my_source = sources[ng]
    flipped = ff_s[my_source]

    loads[0].wait()
    row_ids = lax.broadcasted_iota(jnp.int32, (CELL_ROWS, COLS), 0)

    @pl.loop(0, n_col)
    def _(s):
        hit = row_ids == (cell[s] >> 7)
        rows_1h[:, pl.ds(pl.multiple_of(s * COLS, COLS), COLS)] = jnp.where(
            hit, jnp.float32(1), jnp.float32(0)
        ).astype(jnp.bfloat16)

    acc[...] = jnp.zeros_like(acc)
    loads[6].wait()
    slots = pltpu.make_async_copy(
        mis.at[pl.ds(0, n_col - 1)], mis.at[pl.ds(0, n_col - 1)], a2a_recv
    )
    slots.wait()

    lane_ids = lax.broadcasted_iota(jnp.int32, (COLS, COLS), 0)
    slot_ids = lax.broadcasted_iota(jnp.int32, (1, COLS), 1)

    @pl.loop(0, n_col)
    def _(s):
        value = jnp.where(slot_ids < cnt_s[s], mis[s], jnp.float32(0))
        high = value.astype(jnp.bfloat16).astype(jnp.float32)
        low = value - high
        hit = lane_ids == (cell[s] & 127)
        columns = pl.ds(pl.multiple_of(s * COLS, COLS), COLS)
        vals_1h[0:COLS, columns] = jnp.where(hit, high, jnp.float32(0)).astype(jnp.bfloat16)
        vals_1h[COLS : 2 * COLS, columns] = jnp.where(hit, low, jnp.float32(0)).astype(
            jnp.bfloat16
        )

    width = CHUNK * COLS

    @pl.loop(0, n_col // CHUNK)
    def _(i):
        columns = pl.ds(pl.multiple_of(i * width, width), width)
        acc[...] += lax.dot_general(
            rows_1h[:, columns],
            vals_1h[:, columns],
            (((1,), (1,)), ((), ())),
            preferred_element_type=jnp.float32,
        )

    loads[1].wait()
    forcing = acc[:, :COLS] + acc[:, COLS:]
    y_ref[...] = adj[...] + forcing.reshape(LEVELS, ROWS, COLS)
    for load in loads[2:6]:
        load.wait()

    lanes = lax.broadcasted_iota(jnp.int32, (LEVELS, ROWS, COLS), 2)
    rows = lax.broadcasted_iota(jnp.int32, (LEVELS, ROWS, COLS), 1)
    q_lane = lax.broadcasted_iota(jnp.int32, (VREGS, 8, COLS), 2)
    q_id = lax.broadcasted_iota(jnp.int32, (VREGS, 8, COLS), 0)
    zero = jnp.float32(0)

    for step in range(STEPS):
        line_buf, group_buf = line_bufs[step], group_bufs[step]

        def copy_to(src, dst, send, recv, where):
            return pltpu.make_async_remote_copy(
                src_ref=src,
                dst_ref=dst,
                send_sem=send,
                recv_sem=recv,
                device_id=where,
                device_id_type=MESH,
            )

        y = y_ref[...]
        north = side[2] * y
        south = side[3] * y
        edge_out[step, 0] = north[:, ROWS - 1, :]
        edge_out[step, 1] = south[:, 0, :]
        to_east = side[0] * y
        to_west = side[1] * y
        for way, product, lane in ((0, to_east, COLS - 1), (1, to_west, 0)):
            edge = product.reshape(VREGS, 8, COLS)[:, :, lane : lane + 1]
            col_out[step, way] = jnp.sum(jnp.where(q_lane == q_id, edge, zero), axis=0)

        go_north = copy_to(
            edge_out.at[step, 0],
            edge_in.at[step, 0],
            edge_send.at[step, 0],
            edge_recv.at[step, 0],
            {"tile": t + 1},
        )
        go_south = copy_to(
            edge_out.at[step, 1],
            edge_in.at[step, 1],
            edge_send.at[step, 1],
            edge_recv.at[step, 1],
            {"tile": t - 1},
        )
        go_east = copy_to(
            col_out.at[step, 0],
            col_in.at[step, 0],
            col_send.at[step, 0],
            col_recv.at[step, 0],
            {"col": east},
        )
        go_west = copy_to(
            col_out.at[step, 1],
            col_in.at[step, 1],
            col_send.at[step, 1],
            col_recv.at[step, 1],
            {"col": west},
        )

        @pl.when(t < n_tile - 1)
        def _():
            go_north.start()

        @pl.when(at_top)
        def _():
            line_buf[my_z] = edge_out[step, 0]

            @pl.loop(1, nz)
            def _(i):
                copy_to(
                    edge_out.at[step, 0],
                    line_buf.at[my_z],
                    line_send.at[step],
                    line_recv.at[step],
                    {"col": my_x * nc * nz + ((my_z + i) % nz) * nc + core},
                ).start()

        go_east.start()
        go_west.start()

        @pl.when(t > 0)
        def _():
            go_south.start()

        up = vert[0] * y
        down = vert[1] * y
        level = jnp.zeros((1, ROWS, COLS), jnp.float32)
        r_ref[...] = (
            cen[...] * y
            + jnp.where(lanes == 0, zero, pltpu.roll(to_east, 1, 2))
            + jnp.where(lanes == COLS - 1, zero, pltpu.roll(to_west, COLS - 1, 2))
            + jnp.where(rows == 0, zero, pltpu.roll(north, 1, 1))
            + jnp.where(rows == ROWS - 1, zero, pltpu.roll(south, ROWS - 1, 1))
            + jnp.concatenate([up[1:], level], axis=0)
            + jnp.concatenate([level, down[:-1]], axis=0)
        )

        @pl.when(at_top)
        def _():
            five = pltpu.make_async_copy(
                line_buf.at[pl.ds(0, nz - 1)],
                line_buf.at[pl.ds(0, nz - 1)],
                line_recv.at[step],
            )
            five.wait()
            for g in range(ng):
                picked = line_buf[(sources[g] // nc) % nz]
                pick_buf[step, g] = picked

            @pl.loop(1, ng)
            def _(i):
                g = (my_g + i) % ng
                copy_to(
                    pick_buf.at[step, g],
                    group_buf.at[my_g],
                    pick_send.at[step],
                    pick_recv.at[step],
                    {"col": (g // nc) * nc * nz + my_z * nc + g % nc},
                ).start()

            group_buf[my_g] = pick_buf[step, my_g]
            seven = pltpu.make_async_copy(
                group_buf.at[pl.ds(0, ng - 1)],
                group_buf.at[pl.ds(0, ng - 1)],
                pick_recv.at[step],
            )
            seven.wait()
            arrived = group_buf[(my_source // (nc * nz)) * nc + my_source % nc]
            turn = COLS - 1 - lax.broadcasted_iota(jnp.int32, (LEVELS, COLS), 1)
            turned = jnp.take_along_axis(arrived, turn, axis=1)
            edge_in[step, 1] = jnp.where(flipped == 1, turned, arrived)

        @pl.when(t > 0)
        def _():
            go_north.wait_recv()
            r_ref[:, 0, :] = r_ref[:, 0, :] + edge_in[step, 0]

        @pl.when(t < n_tile - 1)
        def _():
            go_south.wait_recv()

        r_ref[:, ROWS - 1, :] = r_ref[:, ROWS - 1, :] + edge_in[step, 1]

        go_east.wait_recv()
        go_west.wait_recv()
        from_west = jnp.sum(
            jnp.where(q_lane == q_id, col_in[step, 0][None], zero), axis=2, keepdims=True
        ).reshape(LEVELS, ROWS, 1)
        from_east = jnp.sum(
            jnp.where(q_lane == q_id, col_in[step, 1][None], zero), axis=2, keepdims=True
        ).reshape(LEVELS, ROWS, 1)
        sides = jnp.where(lanes == 0, from_west, jnp.where(lanes == COLS - 1, from_east, zero))
        result = (r_ref[...] + sides) * mask[...].astype(jnp.float32)
        if step < STEPS - 1:
            y_ref[...] = result
        else:
            out_ref[...] = result

        @pl.when(t < n_tile - 1)
        def _():
            go_north.wait_send()

        @pl.when(t > 0)
        def _():
            go_south.wait_send()

        go_east.wait_send()
        go_west.wait_send()

        @pl.when(at_top)
        def _():
            pltpu.make_async_copy(
                line_buf.at[pl.ds(0, nz - 1)],
                line_buf.at[pl.ds(0, nz - 1)],
                line_send.at[step],
            ).wait()
            pltpu.make_async_copy(
                group_buf.at[pl.ds(0, ng - 1)],
                group_buf.at[pl.ds(0, ng - 1)],
                pick_send.at[step],
            ).wait()

    pltpu.make_async_copy(
        mis.at[pl.ds(0, n_col - 1)], mis.at[pl.ds(0, n_col - 1)], a2a_send
    ).wait()


def solution(mesh):
    n_tile, n_col = mesh.shape["tile"], mesh.shape["col"]
    nx, nz, nc = grid_of(n_col)
    ng = nx * nc
    cube = (LEVELS, ROWS, COLS)
    f32 = jnp.float32
    any_space = pl.BlockSpec(memory_space=pl.ANY)
    scalars = pl.BlockSpec(memory_space=pltpu.SMEM)
    dma = pltpu.SemaphoreType.DMA

    def body(adj, cen, side, vert, mask, misfit, cell, count, partner, flip):
        return pl.pallas_call(
            functools.partial(kernel, n_tile, n_col),
            out_shape=jax.ShapeDtypeStruct(cube, f32),
            in_specs=[any_space] * 7 + [scalars] * 3,
            out_specs=pl.BlockSpec(memory_space=pltpu.VMEM),
            scratch_shapes=[
                pltpu.VMEM(cube, f32),
                pltpu.VMEM(cube, f32),
                pltpu.VMEM((4,) + cube, f32),
                pltpu.VMEM((2,) + cube, f32),
                pltpu.VMEM(cube, jnp.int32),
                pltpu.VMEM((n_col, 1, COLS), jnp.int32),
                pltpu.VMEM((n_col, 1, COLS), f32),
                pltpu.VMEM((CELL_ROWS, n_col * COLS), jnp.bfloat16),
                pltpu.VMEM((2 * COLS, n_col * COLS), jnp.bfloat16),
                pltpu.VMEM((CELL_ROWS, 2 * COLS), f32),
                pltpu.VMEM(cube, f32),
                pltpu.VMEM(cube, f32),
                pltpu.VMEM((STEPS, 2, LEVELS, COLS), f32),
                pltpu.VMEM((STEPS, 2, LEVELS, COLS), f32),
                pltpu.VMEM((STEPS, 2, 8, COLS), f32),
                pltpu.VMEM((STEPS, 2, 8, COLS), f32),
                [pltpu.VMEM((nz, LEVELS, COLS), f32)] * STEPS,
                pltpu.VMEM((STEPS, ng, LEVELS, COLS), f32),
                [pltpu.VMEM((ng, LEVELS, COLS), f32)] * STEPS,
                dma((7,)),
                dma,
                dma,
                dma((STEPS, 2)),
                dma((STEPS, 2)),
                dma((STEPS, 2)),
                dma((STEPS, 2)),
                dma((STEPS,)),
                dma((STEPS,)),
                dma((STEPS,)),
                dma((STEPS,)),
            ],
            compiler_params=pltpu.CompilerParams(
                collective_id=0, has_side_effects=True, vmem_limit_bytes=60 * 2**20
            ),
        )(
            adj,
            cen,
            side,
            vert,
            mask,
            misfit.reshape(n_col, 1, COLS),
            cell.reshape(n_col, 1, COLS),
            count.reshape(n_col),
            partner,
            flip,
        )

    in_specs = (
        P(None, "tile", "col"),
        P(None, "tile", "col"),
        P(None, None, "tile", "col"),
        P(None, None, "tile", "col"),
        P(None, "tile", "col"),
        P("tile", "col", None, None),
        P("tile", "col", None, None),
        P("tile", "col", None),
        P(),
        P(),
    )
    out_specs = P(None, "tile", "col")
    return jax.shard_map(body, mesh=mesh, in_specs=in_specs, out_specs=out_specs, check_vma=False)
```

```python
import functools

import jax
import jax.numpy as jnp
from jax import lax
from jax.experimental import pallas as pl
from jax.experimental.pallas import tpu as pltpu
from jax.sharding import PartitionSpec as P

LEVELS = 25
ROWS = 32
COLS = 128
CELL_ROWS = LEVELS * ROWS
VREGS = CELL_ROWS // 8
MESH = pl.DeviceIdType.MESH


def grid_of(n_col):
    return (4, 6, 2) if n_col == 48 else (2, n_col // 4, 2)


def copy_to(src, dst, send, recv, where):
    return pltpu.make_async_remote_copy(
        src_ref=src,
        dst_ref=dst,
        send_sem=send,
        recv_sem=recv,
        device_id=where,
        device_id_type=MESH,
    )


def wait_for(ref, sem):
    pltpu.make_async_copy(ref, ref, sem).wait()


def kernel(
    n_tile,
    n_col,
    adj_h,
    cen_h,
    side_h,
    vert_h,
    mask_h,
    mis_h,
    cell_h,
    cnt_s,
    fp_s,
    ff_s,
    out_ref,
    adj,
    cen,
    side,
    vert,
    mask,
    cell,
    plane,
    slots,
    rows_1h,
    vals_1h,
    acc,
    y_ref,
    r_ref,
    fixed_row,
    fixed_col,
    fixed_row_in,
    fixed_col_in,
    row_out,
    row_in,
    col_out,
    col_in,
    corner_out,
    corner_in,
    fold_out,
    fold_in,
    line_bufs,
    pick_bufs,
    group_bufs,
    delta,
    delta_out,
    delta_in,
    load_sem,
    plane_send,
    plane_recv,
    slot_send,
    slot_recv,
    fixed_send,
    fixed_recv,
    halo_send,
    halo_recv,
    line_send,
    line_recv,
    pick_send,
    pick_recv,
    delta_send,
    delta_recv,
):
    nx, nz, nc = grid_of(n_col)
    ng = nx * nc
    f32 = jnp.float32
    zero = f32(0)
    me = lax.axis_index("col")
    t = lax.axis_index("tile")
    core = me % nc
    my_z = (me // nc) % nz
    my_x = me // (nc * nz)
    my_g = my_x * nc + core
    sides = ((me + 1) % n_col, (me + n_col - 1) % n_col)
    tiles = (t + 1, t - 1)
    can_go = (t < n_tile - 1, t > 0)
    can_come = (t > 0, t < n_tile - 1)
    at_top = t == n_tile - 1

    def in_plane(g):
        return (g // nc) * nc * nz + my_z * nc + g % nc

    def on_line(z):
        return my_x * nc * nz + z * nc + core

    loads = [
        pltpu.make_async_copy(src, dst, load_sem.at[i])
        for i, (src, dst) in enumerate(
            [
                (mis_h.at[my_x, :, core], plane.at[my_g]),
                (side_h, side),
                (mask_h, mask),
                (cell_h, cell),
                (adj_h, adj),
                (cen_h, cen),
                (vert_h, vert),
            ]
        )
    ]
    for load in loads:
        load.start()

    for way, outermost in ((0, t < 1), (1, t > n_tile - 2)):

        @pl.when(outermost)
        def _():
            fixed_row_in[way][...] = jnp.zeros((LEVELS, COLS), f32)
            row_in[way][...] = jnp.zeros((2, LEVELS, COLS), f32)
            for across in range(2):
                corner_in[2 * way + across][...] = jnp.zeros((8, COLS), f32)

    barrier = pltpu.get_barrier_semaphore()

    def greet(where):
        pl.semaphore_signal(barrier, inc=1, device_id=where, device_id_type=MESH)

    @pl.loop(1, nz)
    def _(i):
        greet({"col": on_line((my_z + i) % nz)})

    @pl.loop(1, ng)
    def _(i):
        greet({"col": in_plane((my_g + i) % ng)})

    for side_id in sides:
        greet({"col": side_id})
    for way in range(2):

        @pl.when(can_go[way])
        def _():
            greet({"tile": tiles[way]})
            for side_id in sides:
                greet({"tile": tiles[way], "col": side_id})

    pl.semaphore_wait(
        barrier,
        nz - 1 + ng - 1 + 2 + 3 * (jnp.where(t > 0, 1, 0) + jnp.where(t < n_tile - 1, 1, 0)),
    )

    @pl.loop(1, ng)
    def _(i):
        g = (my_g + i) % ng
        copy_to(
            mis_h.at[g // nc, :, g % nc],
            plane.at[my_g],
            plane_send,
            plane_recv,
            {"col": in_plane(g)},
        ).start()

    def find(s, found):
        target = fp_s[s]
        return tuple(jnp.where(target == in_plane(g), s, found[g]) for g in range(ng)) + (
            jnp.where(target == me, s, found[ng]),
        )

    sources = lax.fori_loop(0, n_col, find, (jnp.int32(0),) * (ng + 1))
    my_source = sources[ng]
    flipped = ff_s[my_source]

    lanes = lax.broadcasted_iota(jnp.int32, (LEVELS, ROWS, COLS), 2)
    rows = lax.broadcasted_iota(jnp.int32, (LEVELS, ROWS, COLS), 1)
    q_lane = lax.broadcasted_iota(jnp.int32, (VREGS, 8, COLS), 2)
    q_id = lax.broadcasted_iota(jnp.int32, (VREGS, 8, COLS), 0)
    flat_lane = lax.broadcasted_iota(jnp.int32, (LEVELS, COLS), 1)
    flat_level = lax.broadcasted_iota(jnp.int32, (LEVELS, COLS), 0)
    tile_row = lax.broadcasted_iota(jnp.int32, (8, COLS), 0)
    edge_lane = (COLS - 1, 0)
    land_lane = (0, COLS - 1)
    edge_row = (ROWS - 1, 0)
    land_row = (0, ROWS - 1)

    def pack(cube, lane):
        edge = cube.reshape(VREGS, 8, COLS)[:, :, lane : lane + 1]
        return jnp.sum(jnp.where(q_lane == q_id, edge, zero), axis=0)

    def unpack(tile):
        spread = jnp.where(q_lane == q_id, tile[None], zero)
        return jnp.sum(spread, axis=2, keepdims=True).reshape(LEVELS, ROWS, 1)

    loads[1].wait()
    loads[2].wait()
    ocean = mask[...].astype(f32)
    for way in range(2):
        fixed_col[way][...] = pack(side[way] * ocean, edge_lane[way])
        fixed_row[way][...] = side[2 + way, :, edge_row[way], :] * mask[
            :, edge_row[way], :
        ].astype(f32)
    fixed = [
        copy_to(
            fixed_col[way],
            fixed_col_in[way],
            fixed_send.at[way],
            fixed_recv.at[way],
            {"col": sides[way]},
        )
        for way in range(2)
    ] + [
        copy_to(
            fixed_row[way],
            fixed_row_in[way],
            fixed_send.at[2 + way],
            fixed_recv.at[2 + way],
            {"tile": tiles[way]},
        )
        for way in range(2)
    ]
    for way in range(2):
        fixed[way].start()
        pl.when(can_go[way])(fixed[2 + way].start)

    loads[3].wait()
    row_ids = lax.broadcasted_iota(jnp.int32, (CELL_ROWS, COLS), 0)

    def columns_of(z, g):
        return pl.ds(pl.multiple_of((z * ng + g) * COLS, COLS), COLS)

    @pl.loop(0, nz)
    def _(z):
        for g in range(ng):
            hit = row_ids == (cell[g // nc, z, g % nc] >> 7)
            rows_1h[:, columns_of(z, g)] = jnp.where(hit, f32(1), zero).astype(jnp.bfloat16)

    loads[0].wait()
    wait_for(plane.at[pl.ds(0, ng - 1)], plane_recv)

    for mine in range(nz):

        @pl.when(my_z == mine)
        def _():
            @pl.loop(1, nz)
            def _(i):
                z = (mine + i) % nz
                copy_to(
                    plane.at[:, z],
                    slots[mine],
                    slot_send.at[z],
                    slot_recv.at[mine],
                    {"col": on_line(z)},
                ).start()

            slots[mine][...] = plane[:, mine]

    lane_ids = lax.broadcasted_iota(jnp.int32, (COLS, COLS), 0)
    slot_ids = lax.broadcasted_iota(jnp.int32, (1, COLS), 1)

    def add_slots(z, first):
        @pl.when(my_z != z)
        def _():
            wait_for(slots[z], slot_recv.at[z])

        for g in range(ng):
            count = cnt_s[(g // nc) * nc * nz + z * nc + g % nc]
            value = jnp.where(slot_ids < count, slots[z][g], zero)
            high = value.astype(jnp.bfloat16).astype(f32)
            hit = lane_ids == (cell[g // nc, z, g % nc] & 127)
            for half, part in enumerate((high, value - high)):
                vals_1h[half * COLS : (half + 1) * COLS, g * COLS : (g + 1) * COLS] = jnp.where(
                    hit, part, zero
                ).astype(jnp.bfloat16)
        width = ng * COLS
        term = lax.dot_general(
            rows_1h[:, z * width : (z + 1) * width],
            vals_1h[...],
            (((1,), (1,)), ((), ())),
            preferred_element_type=f32,
        )
        if first:
            acc[...] = term
        else:
            acc[...] += term

    @pl.when(my_z < nz // 2)
    def _():
        for z in range(nz):
            add_slots(z, z == 0)

    @pl.when(my_z >= nz // 2)
    def _():
        for z in range(nz - 1, -1, -1):
            add_slots(z, z == nz - 1)

    loads[4].wait()
    y_ref[...] = adj[...] + (acc[:, :COLS] + acc[:, COLS:]).reshape(LEVELS, ROWS, COLS)

    def fold_start(n):
        line_bufs[n][my_z] = fold_out[n][...]

        @pl.loop(1, nz)
        def _(i):
            copy_to(
                fold_out[n],
                line_bufs[n].at[my_z],
                line_send.at[n],
                line_recv.at[n],
                {"col": on_line((my_z + i) % nz)},
            ).start()

    def fold_pick(n):
        wait_for(line_bufs[n].at[pl.ds(0, nz - 1)], line_recv.at[n])
        for g in range(ng):
            pick_bufs[n][g] = line_bufs[n][(sources[g] // nc) % nz]

        @pl.loop(1, ng)
        def _(i):
            g = (my_g + i) % ng
            copy_to(
                pick_bufs[n].at[g],
                group_bufs[n].at[my_g],
                pick_send.at[n],
                pick_recv.at[n],
                {"col": in_plane(g)},
            ).start()

        group_bufs[n][my_g] = pick_bufs[n][my_g]

    def fold_finish(n):
        wait_for(group_bufs[n].at[pl.ds(0, ng - 1)], pick_recv.at[n])
        arrived = group_bufs[n][(my_source // (nc * nz)) * nc + my_source % nc]
        turned = jnp.take_along_axis(arrived, COLS - 1 - flat_lane, axis=1)
        fold_in[n] = jnp.where(flipped == 1, turned, arrived)

    def interior(y):
        to_east = side[0] * y
        to_west = side[1] * y
        north = side[2] * y
        south = side[3] * y
        up = vert[0] * y
        down = vert[1] * y
        level = jnp.zeros((1, ROWS, COLS), f32)
        r = (
            cen[...] * y
            + jnp.where(lanes == 0, zero, pltpu.roll(to_east, 1, 2))
            + jnp.where(lanes == COLS - 1, zero, pltpu.roll(to_west, COLS - 1, 2))
            + jnp.where(rows == 0, zero, pltpu.roll(north, 1, 1))
            + jnp.where(rows == ROWS - 1, zero, pltpu.roll(south, ROWS - 1, 1))
            + jnp.concatenate([up[1:], level], axis=0)
            + jnp.concatenate([level, down[:-1]], axis=0)
        )
        return r

    for load in loads[5:]:
        load.wait()

    @pl.when(at_top)
    def _():
        fold_out[0][...] = side[2, :, ROWS - 1, :] * y_ref[:, ROWS - 1, :]
        fold_start(0)

    r_ref[...] = interior(y_ref[...])
    for way in range(2):
        col_out[way][0] = pack(side[way] * y_ref[...], edge_lane[way])
        col_out[way][1] = fixed_col[way][...] * pack(r_ref[...], edge_lane[way])
        at = edge_row[way]
        row_out[way][0] = side[2 + way, :, at, :] * y_ref[:, at, :]
        row_out[way][1] = fixed_row[way][...] * r_ref[:, at, :]
        for across in range(2):
            lane = edge_lane[across]
            spot = flat_lane == 4 * flat_level + 3 * way
            level_value = y_ref[:, at, :][:, lane : lane + 1]
            for part, weight in enumerate((side[2 + way, :, at, :], side[across, :, at, :])):
                term = weight[:, lane : lane + 1] * level_value
                corner_out[2 * way + across][part : part + 1, :] = jnp.sum(
                    jnp.where(spot, term, zero), axis=0, keepdims=True
                )

    halos = []
    for way in range(2):
        halos.append(
            copy_to(
                col_out[way],
                col_in[way],
                halo_send.at[way],
                halo_recv.at[way],
                {"col": sides[way]},
            )
        )
        halos[-1].start()
    far = []
    for way in range(2):
        far.append(
            [
                copy_to(
                    row_out[way],
                    row_in[way],
                    halo_send.at[2 + way],
                    halo_recv.at[2 + way],
                    {"tile": tiles[way]},
                )
            ]
            + [
                copy_to(
                    corner_out[2 * way + across],
                    corner_in[2 * way + across],
                    halo_send.at[4 + 2 * way + across],
                    halo_recv.at[4 + 2 * way + across],
                    {"tile": tiles[way], "col": sides[across]},
                )
                for across in range(2)
            ]
        )

        @pl.when(can_go[way])
        def _():
            for copy in far[way]:
                copy.start()

    for way in range(2):
        halos[way].wait_recv()
        fixed[way].wait_recv()

        @pl.when(can_come[way])
        def _():
            fixed[2 + way].wait_recv()
            for copy in far[way]:
                copy.wait_recv()

    def with_sides(r, west, east):
        return r + jnp.where(lanes == 0, west, jnp.where(lanes == COLS - 1, east, zero))

    for way in range(2):
        at = land_row[way]
        r_ref[:, at, :] = r_ref[:, at, :] + row_in[way][0]
    y_ref[...] = with_sides(r_ref[...], unpack(col_in[0][0]), unpack(col_in[1][0])) * mask[
        ...
    ].astype(f32)

    ring = []
    for across in range(2):
        lacked = col_out[1 - across][0]
        for way, sub in ((0, 0), (1, 7)):
            lacked = lacked + jnp.where(tile_row == sub, corner_in[2 * way + across][0:1, :], zero)
        ring.append(col_in[across][1] + fixed_col_in[across][...] * lacked)
    r_ref[...] = with_sides(interior(y_ref[...]), unpack(ring[0]), unpack(ring[1]))
    for way in range(2):
        lacked = row_out[1 - way][0]
        for across in range(2):
            spot = flat_lane == 4 * flat_level + 3 * way
            term = jnp.sum(
                jnp.where(spot, corner_in[2 * way + across][1:2, :], zero), axis=1, keepdims=True
            )
            lacked = lacked + jnp.where(flat_lane == land_lane[across], term, zero)
        at = land_row[way]
        r_ref[:, at, :] = r_ref[:, at, :] + (row_in[way][1] + fixed_row_in[way][...] * lacked)
    out_ref[...] = r_ref[...] * mask[...].astype(f32)

    @pl.when(at_top)
    def _():
        top = ROWS - 1
        fold_pick(0)
        fold_finish(0)
        delta[...] = fold_in[0] * mask[:, top, :].astype(f32)
        fold_out[1][...] = side[2, :, top, :] * (y_ref[:, top, :] + delta[...])
        fold_start(1)
        moves = []
        for way in range(2):
            delta_out[way][...] = side[way, :, top, :] * delta[...]
            moves.append(
                copy_to(
                    delta_out[way],
                    delta_in[way],
                    delta_send.at[way],
                    delta_recv.at[way],
                    {"col": sides[way]},
                )
            )
            moves[way].start()
        level = jnp.zeros((1, COLS), f32)
        up = vert[0, :, top, :] * delta[...]
        down = vert[1, :, top, :] * delta[...]
        change = (
            cen[:, top, :] * delta[...]
            + jnp.concatenate([up[1:], level], axis=0)
            + jnp.concatenate([level, down[:-1]], axis=0)
        )
        for way in range(2):
            moves[way].wait_recv()
            shift = 1 if way == 0 else COLS - 1
            change = change + jnp.where(
                flat_lane == land_lane[way],
                pltpu.roll(delta_in[way][...], shift, 1),
                pltpu.roll(delta_out[way][...], shift, 1),
            )
        below = side[3, :, top, :] * delta[...]
        out_ref[:, top - 1, :] = out_ref[:, top - 1, :] + below * mask[:, top - 1, :].astype(f32)
        fold_pick(1)
        fold_finish(1)
        change = change + fold_in[1]
        out_ref[:, top, :] = out_ref[:, top, :] + change * mask[:, top, :].astype(f32)
        for way in range(2):
            moves[way].wait_send()
            wait_for(line_bufs[way].at[pl.ds(0, nz - 1)], line_send.at[way])
            wait_for(group_bufs[way].at[pl.ds(0, ng - 1)], pick_send.at[way])

    wait_for(plane.at[pl.ds(0, ng - 1)], plane_send)

    @pl.loop(1, nz)
    def _(i):
        wait_for(slots[0], slot_send.at[(my_z + i) % nz])

    for way in range(2):
        halos[way].wait_send()
        fixed[way].wait_send()

        @pl.when(can_go[way])
        def _():
            fixed[2 + way].wait_send()
            for copy in far[way]:
                copy.wait_send()


def solution(mesh):
    n_tile, n_col = mesh.shape["tile"], mesh.shape["col"]
    nx, nz, nc = grid_of(n_col)
    ng = nx * nc
    cube = (LEVELS, ROWS, COLS)
    flat = (LEVELS, COLS)
    f32 = jnp.float32
    any_space = pl.BlockSpec(memory_space=pl.ANY)
    scalars = pl.BlockSpec(memory_space=pltpu.SMEM)
    dma = pltpu.SemaphoreType.DMA

    def body(adj, cen, side, vert, mask, misfit, cell, count, partner, flip):
        return pl.pallas_call(
            functools.partial(kernel, n_tile, n_col),
            out_shape=jax.ShapeDtypeStruct(cube, f32),
            in_specs=[any_space] * 7 + [scalars] * 3,
            out_specs=pl.BlockSpec(memory_space=pltpu.VMEM),
            scratch_shapes=[
                pltpu.VMEM(cube, f32),
                pltpu.VMEM(cube, f32),
                pltpu.VMEM((4,) + cube, f32),
                pltpu.VMEM((2,) + cube, f32),
                pltpu.VMEM(cube, jnp.int32),
                pltpu.VMEM((nx, nz, nc, 1, COLS), jnp.int32),
                pltpu.VMEM((ng, nz, 1, COLS), f32),
                [pltpu.VMEM((ng, 1, COLS), f32)] * nz,
                pltpu.VMEM((CELL_ROWS, n_col * COLS), jnp.bfloat16),
                pltpu.VMEM((2 * COLS, ng * COLS), jnp.bfloat16),
                pltpu.VMEM((CELL_ROWS, 2 * COLS), f32),
                pltpu.VMEM(cube, f32),
                pltpu.VMEM(cube, f32),
                [pltpu.VMEM(flat, f32)] * 2,
                [pltpu.VMEM((8, COLS), f32)] * 2,
                [pltpu.VMEM(flat, f32)] * 2,
                [pltpu.VMEM((8, COLS), f32)] * 2,
                [pltpu.VMEM((2,) + flat, f32)] * 2,
                [pltpu.VMEM((2,) + flat, f32)] * 2,
                [pltpu.VMEM((2, 8, COLS), f32)] * 2,
                [pltpu.VMEM((2, 8, COLS), f32)] * 2,
                [pltpu.VMEM((8, COLS), f32)] * 4,
                [pltpu.VMEM((8, COLS), f32)] * 4,
                [pltpu.VMEM(flat, f32)] * 2,
                pltpu.VMEM((2,) + flat, f32),
                [pltpu.VMEM((nz,) + flat, f32)] * 2,
                [pltpu.VMEM((ng,) + flat, f32)] * 2,
                [pltpu.VMEM((ng,) + flat, f32)] * 2,
                pltpu.VMEM(flat, f32),
                [pltpu.VMEM(flat, f32)] * 2,
                [pltpu.VMEM(flat, f32)] * 2,
                dma((7,)),
                dma,
                dma,
                dma((nz,)),
                dma((nz,)),
                dma((4,)),
                dma((4,)),
                dma((8,)),
                dma((8,)),
                dma((2,)),
                dma((2,)),
                dma((2,)),
                dma((2,)),
                dma((2,)),
                dma((2,)),
            ],
            compiler_params=pltpu.CompilerParams(
                collective_id=0, has_side_effects=True, vmem_limit_bytes=60 * 2**20
            ),
        )(
            adj,
            cen,
            side,
            vert,
            mask,
            misfit.reshape(nx, nz, nc, 1, COLS),
            cell.reshape(nx, nz, nc, 1, COLS),
            count.reshape(n_col),
            partner,
            flip,
        )

    in_specs = (
        P(None, "tile", "col"),
        P(None, "tile", "col"),
        P(None, None, "tile", "col"),
        P(None, None, "tile", "col"),
        P(None, "tile", "col"),
        P("tile", "col", None, None),
        P("tile", "col", None, None),
        P("tile", "col", None),
        P(),
        P(),
    )
    out_specs = P(None, "tile", "col")
    return jax.shard_map(body, mesh=mesh, in_specs=in_specs, out_specs=out_specs, check_vma=False)
```

```python
import functools

import jax
import jax.numpy as jnp
from jax import lax
from jax.experimental import pallas as pl
from jax.experimental.pallas import tpu as pltpu
from jax.sharding import PartitionSpec as P

LEVELS = 25
ROWS = 32
COLS = 128
CELL_ROWS = LEVELS * ROWS
VREGS = CELL_ROWS // 8
PARTS = ((0, 16), (16, LEVELS))
MESH = pl.DeviceIdType.MESH


def grid_of(n_col):
    return (4, 6, 2) if n_col == 48 else (2, n_col // 4, 2)


def copy_to(src, dst, send, recv, where):
    return pltpu.make_async_remote_copy(
        src_ref=src,
        dst_ref=dst,
        send_sem=send,
        recv_sem=recv,
        device_id=where,
        device_id_type=MESH,
    )


def wait_for(ref, sem):
    pltpu.make_async_copy(ref, ref, sem).wait()


def hand_out(result, out_h, sem):
    copy = pltpu.make_async_copy(result, out_h, sem)
    copy.start()
    copy.wait()


def kernel(
    n_tile,
    n_col,
    adj_h,
    cen_h,
    side_h,
    vert_h,
    mask_h,
    mis_h,
    cell_h,
    cnt_s,
    fp_s,
    ff_s,
    out_ref,
    adj,
    cen,
    side,
    vert,
    mask,
    cell,
    plane,
    slots,
    rows_1h,
    vals_1h,
    acc,
    y_ref,
    r_ref,
    fixed_row,
    fixed_col,
    fixed_row_in,
    fixed_col_in,
    row_out,
    row_in,
    col_out,
    col_in,
    corner_out,
    corner_in,
    fold_out,
    line_bufs,
    pick_bufs,
    group_bufs,
    top_1h,
    delta,
    delta_out,
    delta_in,
    load_sem,
    plane_send,
    plane_recv,
    slot_send,
    slot_recv,
    fixed_send,
    fixed_recv,
    halo_send,
    halo_recv,
    line_send,
    line_recv,
    pick_send,
    pick_recv,
    delta_send,
    delta_recv,
):
    nx, nz, nc = grid_of(n_col)
    ng = nx * nc
    f32 = jnp.float32
    zero = f32(0)
    me = lax.axis_index("col")
    t = lax.axis_index("tile")
    core = me % nc
    my_z = (me // nc) % nz
    my_x = me // (nc * nz)
    my_g = my_x * nc + core
    sides = ((me + 1) % n_col, (me + n_col - 1) % n_col)
    tiles = (t + 1, t - 1)
    can_go = (t < n_tile - 1, t > 0)
    can_come = (t > 0, t < n_tile - 1)
    at_top = t == n_tile - 1

    def in_plane(g):
        return (g // nc) * nc * nz + my_z * nc + g % nc

    def on_line(z):
        return my_x * nc * nz + z * nc + core

    loads = [
        pltpu.make_async_copy(src, dst, load_sem.at[i])
        for i, (src, dst) in enumerate(
            [
                (mis_h.at[my_x, :, core], plane.at[my_g]),
                (side_h, side),
                (mask_h, mask),
                (cell_h, cell),
                (adj_h, adj),
                (cen_h, cen),
                (vert_h, vert),
            ]
        )
    ]
    for load in loads:
        load.start()

    for way, outermost in ((0, t < 1), (1, t > n_tile - 2)):

        @pl.when(outermost)
        def _():
            fixed_row_in[way][...] = jnp.zeros((LEVELS, COLS), f32)
            row_in[way][...] = jnp.zeros((2, LEVELS, COLS), f32)
            for across in range(2):
                corner_in[2 * way + across][...] = jnp.zeros((8, COLS), f32)

    barrier = pltpu.get_barrier_semaphore()

    def greet(where):
        pl.semaphore_signal(barrier, inc=1, device_id=where, device_id_type=MESH)

    @pl.loop(1, nz)
    def _(i):
        greet({"col": on_line((my_z + i) % nz)})

    @pl.loop(1, ng)
    def _(i):
        greet({"col": in_plane((my_g + i) % ng)})

    for side_id in sides:
        greet({"col": side_id})
    for way in range(2):

        @pl.when(can_go[way])
        def _():
            greet({"tile": tiles[way]})
            for side_id in sides:
                greet({"tile": tiles[way], "col": side_id})

    pl.semaphore_wait(
        barrier,
        nz - 1 + ng - 1 + 2 + 3 * (jnp.where(t > 0, 1, 0) + jnp.where(t < n_tile - 1, 1, 0)),
    )

    far_way = 1 - 2 * (my_z // (nz // 2))

    @pl.loop(1, ng)
    def _(i):
        g = (my_g + i) % ng
        copy_to(
            mis_h.at[g // nc, :, g % nc],
            plane.at[my_g],
            plane_send,
            plane_recv,
            {"col": in_plane(g)},
        ).start()

    def find(s, found):
        target = fp_s[s]
        return tuple(jnp.where(target == in_plane(g), s, found[g]) for g in range(ng)) + (
            jnp.where(target == me, s, found[ng]),
        )

    sources = lax.fori_loop(0, n_col, find, (jnp.int32(0),) * (ng + 1))
    my_source = sources[ng]
    flipped = ff_s[my_source]

    lanes = lax.broadcasted_iota(jnp.int32, (LEVELS, ROWS, COLS), 2)
    rows = lax.broadcasted_iota(jnp.int32, (LEVELS, ROWS, COLS), 1)
    q_lane = lax.broadcasted_iota(jnp.int32, (VREGS, 8, COLS), 2)
    q_id = lax.broadcasted_iota(jnp.int32, (VREGS, 8, COLS), 0)
    flat_lane = lax.broadcasted_iota(jnp.int32, (LEVELS, COLS), 1)
    flat_level = lax.broadcasted_iota(jnp.int32, (LEVELS, COLS), 0)
    tile_row = lax.broadcasted_iota(jnp.int32, (8, COLS), 0)
    edge_lane = (COLS - 1, 0)
    land_lane = (0, COLS - 1)
    edge_row = (ROWS - 1, 0)
    land_row = (0, ROWS - 1)

    def pack(cube, lane):
        edge = cube.reshape(VREGS, 8, COLS)[:, :, lane : lane + 1]
        return jnp.sum(jnp.where(q_lane == q_id, edge, zero), axis=0)

    def unpack(tile):
        spread = jnp.where(q_lane == q_id, tile[None], zero)
        return jnp.sum(spread, axis=2, keepdims=True).reshape(LEVELS, ROWS, 1)

    loads[1].wait()
    loads[2].wait()
    ocean = mask[...].astype(f32)
    for way in range(2):
        fixed_col[way][...] = pack(side[way] * ocean, edge_lane[way])
        fixed_row[way][...] = side[2 + way, :, edge_row[way], :] * mask[
            :, edge_row[way], :
        ].astype(f32)
    fixed = [
        copy_to(
            fixed_col[way],
            fixed_col_in[way],
            fixed_send.at[way],
            fixed_recv.at[way],
            {"col": sides[way]},
        )
        for way in range(2)
    ] + [
        copy_to(
            fixed_row[way],
            fixed_row_in[way],
            fixed_send.at[2 + way],
            fixed_recv.at[2 + way],
            {"tile": tiles[way]},
        )
        for way in range(2)
    ]
    for way in range(2):
        fixed[way].start()
        pl.when(can_go[way])(fixed[2 + way].start)

    loads[3].wait()
    row_ids = lax.broadcasted_iota(jnp.int32, (CELL_ROWS, COLS), 0)

    def columns_of(z, g):
        return pl.ds(pl.multiple_of((z * ng + g) * COLS, COLS), COLS)

    @pl.loop(0, nz)
    def _(z):
        for g in range(ng):
            hit = row_ids == (cell[g // nc, z, g % nc] >> 7)
            rows_1h[:, columns_of(z, g)] = jnp.where(hit, f32(1), zero).astype(jnp.bfloat16)

    loads[0].wait()
    wait_for(plane.at[pl.ds(0, ng - 1)], plane_recv)

    for mine in range(nz):

        @pl.when(my_z == mine)
        def _():
            @pl.loop(1, nz)
            def _(i):
                z = (mine + i) % nz
                copy_to(
                    plane.at[:, z],
                    slots[mine],
                    slot_send.at[z],
                    slot_recv.at[mine],
                    {"col": on_line(z)},
                ).start()

            slots[mine][...] = plane[:, mine]

    lane_ids = lax.broadcasted_iota(jnp.int32, (COLS, COLS), 0)
    slot_ids = lax.broadcasted_iota(jnp.int32, (1, COLS), 1)

    def fold_start(n, h):
        part = 2 * n + h
        line_bufs[part][my_z] = fold_out[part][...]

        @pl.loop(1, nz)
        def _(i):
            z = (my_z + nz + far_way * (nz - i)) % nz
            copy_to(
                fold_out[part],
                line_bufs[part].at[my_z],
                line_send.at[part],
                line_recv.at[part],
                {"col": on_line(z)},
            ).start()

    def fold_pick(n, h):
        part = 2 * n + h
        wait_for(line_bufs[part].at[pl.ds(0, nz - 1)], line_recv.at[part])
        for g in range(ng):
            pick_bufs[part][g] = line_bufs[part][(sources[g] // nc) % nz]

        @pl.loop(1, ng)
        def _(i):
            g = (my_g + i) % ng
            copy_to(
                pick_bufs[part].at[g],
                group_bufs[part].at[my_g],
                pick_send.at[part],
                pick_recv.at[part],
                {"col": in_plane(g)},
            ).start()

        group_bufs[part][my_g] = pick_bufs[part][my_g]

    def fold_finish(n, h):
        part = 2 * n + h
        count = PARTS[h][1] - PARTS[h][0]
        wait_for(group_bufs[part].at[pl.ds(0, ng - 1)], pick_recv.at[part])
        arrived = group_bufs[part][(my_source // (nc * nz)) * nc + my_source % nc]
        backwards = COLS - 1 - lax.broadcasted_iota(jnp.int32, (count, COLS), 1)
        turned = jnp.take_along_axis(arrived, backwards, axis=1)
        return jnp.where(flipped == 1, turned, arrived)

    for load in loads[4:]:
        load.wait()

    def add_slots(z, first, last):
        @pl.when(my_z != z)
        def _():
            wait_for(slots[z], slot_recv.at[z])

        for g in range(ng):
            count = cnt_s[(g // nc) * nc * nz + z * nc + g % nc]
            value = jnp.where(slot_ids < count, slots[z][g], zero)
            high = value.astype(jnp.bfloat16).astype(f32)
            hit = lane_ids == (cell[g // nc, z, g % nc] & 127)
            for half, part in enumerate((high, value - high)):
                vals_1h[half * COLS : (half + 1) * COLS, g * COLS : (g + 1) * COLS] = jnp.where(
                    hit, part, zero
                ).astype(jnp.bfloat16)

        def lead():
            level_ids = lax.broadcasted_iota(jnp.int32, (ROWS, COLS), 0)
            for g in range(ng):
                cell_row = cell[g // nc, z, g % nc] >> 7
                level = jnp.where((cell_row & (ROWS - 1)) == ROWS - 1, cell_row >> 5, -1)
                top_1h[:, g * COLS : (g + 1) * COLS] = jnp.where(
                    level_ids == level, f32(1), zero
                ).astype(jnp.bfloat16)
            row = lax.dot_general(
                top_1h[...],
                vals_1h[...],
                (((1,), (1,)), ((), ())),
                preferred_element_type=f32,
            )[:LEVELS]
            row = row + acc[...].reshape(LEVELS, ROWS, 2 * COLS)[:, ROWS - 1, :]
            row = adj[:, ROWS - 1, :] + row[:, :COLS] + row[:, COLS:]
            for h, (low, high) in enumerate(PARTS):
                fold_out[h][...] = side[2, low:high, ROWS - 1, :] * row[low:high]
                fold_start(0, h)

        if last:
            pl.when(at_top)(lead)
        width = ng * COLS
        term = lax.dot_general(
            rows_1h[:, z * width : (z + 1) * width],
            vals_1h[...],
            (((1,), (1,)), ((), ())),
            preferred_element_type=f32,
        )
        if first:
            acc[...] = term
        else:
            acc[...] += term

    @pl.when(my_z < nz // 2)
    def _():
        for z in range(nz):
            add_slots(z, z == 0, z == nz - 1)

    @pl.when(my_z >= nz // 2)
    def _():
        for z in range(nz - 1, -1, -1):
            add_slots(z, z == nz - 1, z == 0)

    y_ref[...] = adj[...] + (acc[:, :COLS] + acc[:, COLS:]).reshape(LEVELS, ROWS, COLS)

    def interior(y):
        to_east = side[0] * y
        to_west = side[1] * y
        north = side[2] * y
        south = side[3] * y
        up = vert[0] * y
        down = vert[1] * y
        level = jnp.zeros((1, ROWS, COLS), f32)
        r = (
            cen[...] * y
            + jnp.where(lanes == 0, zero, pltpu.roll(to_east, 1, 2))
            + jnp.where(lanes == COLS - 1, zero, pltpu.roll(to_west, COLS - 1, 2))
            + jnp.where(rows == 0, zero, pltpu.roll(north, 1, 1))
            + jnp.where(rows == ROWS - 1, zero, pltpu.roll(south, ROWS - 1, 1))
            + jnp.concatenate([up[1:], level], axis=0)
            + jnp.concatenate([level, down[:-1]], axis=0)
        )
        return r

    r_ref[...] = interior(y_ref[...])
    for way in range(2):
        col_out[way][0] = pack(side[way] * y_ref[...], edge_lane[way])
        col_out[way][1] = fixed_col[way][...] * pack(r_ref[...], edge_lane[way])
        at = edge_row[way]
        row_out[way][0] = side[2 + way, :, at, :] * y_ref[:, at, :]
        row_out[way][1] = fixed_row[way][...] * r_ref[:, at, :]
        for across in range(2):
            lane = edge_lane[across]
            spot = flat_lane == 4 * flat_level + 3 * way
            level_value = y_ref[:, at, :][:, lane : lane + 1]
            for part, weight in enumerate((side[2 + way, :, at, :], side[across, :, at, :])):
                term = weight[:, lane : lane + 1] * level_value
                corner_out[2 * way + across][part : part + 1, :] = jnp.sum(
                    jnp.where(spot, term, zero), axis=0, keepdims=True
                )

    halos = []
    for way in range(2):
        halos.append(
            copy_to(
                col_out[way],
                col_in[way],
                halo_send.at[way],
                halo_recv.at[way],
                {"col": sides[way]},
            )
        )
        halos[-1].start()
    far = []
    for way in range(2):
        far.append(
            [
                copy_to(
                    row_out[way],
                    row_in[way],
                    halo_send.at[2 + way],
                    halo_recv.at[2 + way],
                    {"tile": tiles[way]},
                )
            ]
            + [
                copy_to(
                    corner_out[2 * way + across],
                    corner_in[2 * way + across],
                    halo_send.at[4 + 2 * way + across],
                    halo_recv.at[4 + 2 * way + across],
                    {"tile": tiles[way], "col": sides[across]},
                )
                for across in range(2)
            ]
        )

        @pl.when(can_go[way])
        def _():
            for copy in far[way]:
                copy.start()

    @pl.when(at_top)
    def _():
        for h in range(2):
            fold_pick(0, h)

    for way in range(2):
        halos[way].wait_recv()
        fixed[way].wait_recv()

        @pl.when(can_come[way])
        def _():
            fixed[2 + way].wait_recv()
            for copy in far[way]:
                copy.wait_recv()

    def with_sides(r, west, east):
        return r + jnp.where(lanes == 0, west, jnp.where(lanes == COLS - 1, east, zero))

    for way in range(2):
        at = land_row[way]
        r_ref[:, at, :] = r_ref[:, at, :] + row_in[way][0]
    y_ref[...] = with_sides(r_ref[...], unpack(col_in[0][0]), unpack(col_in[1][0])) * mask[
        ...
    ].astype(f32)

    top = ROWS - 1
    moves = [
        copy_to(
            delta_out[way],
            delta_in[way],
            delta_send.at[way],
            delta_recv.at[way],
            {"col": sides[way]},
        )
        for way in range(2)
    ]

    @pl.when(at_top)
    def _():
        for h, (low, high) in enumerate(PARTS):
            edge = mask[low:high, top, :].astype(f32) * fold_finish(0, h)
            delta[low:high, :] = edge
            fold_out[2 + h][...] = side[2, low:high, top, :] * (y_ref[low:high, top, :] + edge)
            fold_start(1, h)
        for way in range(2):
            delta_out[way][...] = side[way, :, top, :] * delta[...]
            moves[way].start()

    ring = []
    for across in range(2):
        lacked = col_out[1 - across][0]
        for way, sub in ((0, 0), (1, 7)):
            lacked = lacked + jnp.where(tile_row == sub, corner_in[2 * way + across][0:1, :], zero)
        ring.append(col_in[across][1] + fixed_col_in[across][...] * lacked)
    r_ref[...] = with_sides(interior(y_ref[...]), unpack(ring[0]), unpack(ring[1]))
    for way in range(2):
        lacked = row_out[1 - way][0]
        for across in range(2):
            spot = flat_lane == 4 * flat_level + 3 * way
            term = jnp.sum(
                jnp.where(spot, corner_in[2 * way + across][1:2, :], zero), axis=1, keepdims=True
            )
            lacked = lacked + jnp.where(flat_lane == land_lane[across], term, zero)
        at = land_row[way]
        r_ref[:, at, :] = r_ref[:, at, :] + (row_in[way][1] + fixed_row_in[way][...] * lacked)
    out_ref[...] = r_ref[...] * mask[...].astype(f32)

    @pl.when(at_top)
    def _():
        level = jnp.zeros((1, COLS), f32)
        up = vert[0, :, top, :] * delta[...]
        down = vert[1, :, top, :] * delta[...]
        change = (
            cen[:, top, :] * delta[...]
            + jnp.concatenate([up[1:], level], axis=0)
            + jnp.concatenate([level, down[:-1]], axis=0)
        )
        for way in range(2):
            moves[way].wait_recv()
            shift = 1 if way == 0 else COLS - 1
            change = change + jnp.where(
                flat_lane == land_lane[way],
                pltpu.roll(delta_in[way][...], shift, 1),
                pltpu.roll(delta_out[way][...], shift, 1),
            )
        below = side[3, :, top, :] * delta[...]
        out_ref[:, top - 1, :] = out_ref[:, top - 1, :] + below * mask[:, top - 1, :].astype(f32)
        delta[...] = change
        for h in range(2):
            fold_pick(1, h)
        for h, (low, high) in enumerate(PARTS):
            total = delta[low:high, :] + fold_finish(1, h)
            out_ref[low:high, top, :] = out_ref[low:high, top, :] + total * mask[
                low:high, top, :
            ].astype(f32)
        for way in range(2):
            moves[way].wait_send()
        for part in range(4):
            wait_for(line_bufs[part].at[pl.ds(0, nz - 1)], line_send.at[part])
            wait_for(group_bufs[part].at[pl.ds(0, ng - 1)], pick_send.at[part])

    wait_for(plane.at[pl.ds(0, ng - 1)], plane_send)

    @pl.loop(1, nz)
    def _(i):
        wait_for(slots[0], slot_send.at[(my_z + i) % nz])

    for way in range(2):
        halos[way].wait_send()
        fixed[way].wait_send()

        @pl.when(can_go[way])
        def _():
            fixed[2 + way].wait_send()
            for copy in far[way]:
                copy.wait_send()


def solution(mesh):
    n_tile, n_col = mesh.shape["tile"], mesh.shape["col"]
    nx, nz, nc = grid_of(n_col)
    ng = nx * nc
    cube = (LEVELS, ROWS, COLS)
    flat = (LEVELS, COLS)
    parts = [(high - low, COLS) for low, high in PARTS] * 2
    f32 = jnp.float32
    any_space = pl.BlockSpec(memory_space=pl.ANY)
    scalars = pl.BlockSpec(memory_space=pltpu.SMEM)
    dma = pltpu.SemaphoreType.DMA

    def body(adj, cen, side, vert, mask, misfit, cell, count, partner, flip):
        result = pl.pallas_call(
            functools.partial(kernel, n_tile, n_col),
            out_shape=pltpu.VMEM(cube, f32),
            in_specs=[any_space] * 7 + [scalars] * 3,
            out_specs=pl.BlockSpec(memory_space=pltpu.VMEM),
            scratch_shapes=[
                pltpu.VMEM(cube, f32),
                pltpu.VMEM(cube, f32),
                pltpu.VMEM((4,) + cube, f32),
                pltpu.VMEM((2,) + cube, f32),
                pltpu.VMEM(cube, jnp.int32),
                pltpu.VMEM((nx, nz, nc, 1, COLS), jnp.int32),
                pltpu.VMEM((ng, nz, 1, COLS), f32),
                [pltpu.VMEM((ng, 1, COLS), f32)] * nz,
                pltpu.VMEM((CELL_ROWS, n_col * COLS), jnp.bfloat16),
                pltpu.VMEM((2 * COLS, ng * COLS), jnp.bfloat16),
                pltpu.VMEM((CELL_ROWS, 2 * COLS), f32),
                pltpu.VMEM(cube, f32),
                pltpu.VMEM(cube, f32),
                [pltpu.VMEM(flat, f32)] * 2,
                [pltpu.VMEM((8, COLS), f32)] * 2,
                [pltpu.VMEM(flat, f32)] * 2,
                [pltpu.VMEM((8, COLS), f32)] * 2,
                [pltpu.VMEM((2,) + flat, f32)] * 2,
                [pltpu.VMEM((2,) + flat, f32)] * 2,
                [pltpu.VMEM((2, 8, COLS), f32)] * 2,
                [pltpu.VMEM((2, 8, COLS), f32)] * 2,
                [pltpu.VMEM((8, COLS), f32)] * 4,
                [pltpu.VMEM((8, COLS), f32)] * 4,
                [pltpu.VMEM(part, f32) for part in parts],
                [pltpu.VMEM((nz,) + part, f32) for part in parts],
                [pltpu.VMEM((ng,) + part, f32) for part in parts],
                [pltpu.VMEM((ng,) + part, f32) for part in parts],
                pltpu.VMEM((ROWS, ng * COLS), jnp.bfloat16),
                pltpu.VMEM(flat, f32),
                [pltpu.VMEM(flat, f32)] * 2,
                [pltpu.VMEM(flat, f32)] * 2,
                dma((7,)),
                dma,
                dma,
                dma((nz,)),
                dma((nz,)),
                dma((4,)),
                dma((4,)),
                dma((8,)),
                dma((8,)),
                dma((4,)),
                dma((4,)),
                dma((4,)),
                dma((4,)),
                dma((2,)),
                dma((2,)),
            ],
            compiler_params=pltpu.CompilerParams(
                collective_id=0, has_side_effects=True, vmem_limit_bytes=60 * 2**20
            ),
        )(
            adj,
            cen,
            side,
            vert,
            mask,
            misfit.reshape(nx, nz, nc, 1, COLS),
            cell.reshape(nx, nz, nc, 1, COLS),
            count.reshape(n_col),
            partner,
            flip,
        )
        return pl.pallas_call(
            hand_out,
            out_shape=jax.ShapeDtypeStruct(cube, f32),
            in_specs=[pl.BlockSpec(memory_space=pltpu.VMEM)],
            out_specs=any_space,
            scratch_shapes=[dma],
            compiler_params=pltpu.CompilerParams(vmem_limit_bytes=2**20),
        )(result)

    in_specs = (
        P(None, "tile", "col"),
        P(None, "tile", "col"),
        P(None, None, "tile", "col"),
        P(None, None, "tile", "col"),
        P(None, "tile", "col"),
        P("tile", "col", None, None),
        P("tile", "col", None, None),
        P("tile", "col", None),
        P(),
        P(),
    )
    out_specs = P(None, "tile", "col")
    return jax.shard_map(body, mesh=mesh, in_specs=in_specs, out_specs=out_specs, check_vma=False)
```

```python
import functools

import jax
import jax.numpy as jnp
from jax import lax
from jax.experimental import pallas as pl
from jax.experimental.pallas import tpu as pltpu
from jax.sharding import PartitionSpec as P

LEVELS = 25
ROWS = 32
COLS = 128
CELL_ROWS = LEVELS * ROWS
VREGS = CELL_ROWS // 8
PARTS = ((0, 16), (16, LEVELS))
MESH = pl.DeviceIdType.MESH


def grid_of(n_col):
    return (4, 6, 2) if n_col == 48 else (2, n_col // 4, 2)


def nearest_first(z, nz):
    short = z * (nz - 1 - z) // 3
    longer = 1 - 2 * (z // (nz // 2))
    order = []
    for k in range(nz):
        both = (k + 1) // 2 * (1 if k % 2 else -1)
        two_sided = (2 * short - k + nz) // nz
        order.append(z + longer * (two_sided * both + (1 - two_sided) * (k - short)))
    return order


def copy_to(src, dst, send, recv, where):
    return pltpu.make_async_remote_copy(
        src_ref=src,
        dst_ref=dst,
        send_sem=send,
        recv_sem=recv,
        device_id=where,
        device_id_type=MESH,
    )


def wait_for(ref, sem):
    pltpu.make_async_copy(ref, ref, sem).wait()


def hand_out(result, out_h, sem):
    copy = pltpu.make_async_copy(result, out_h, sem)
    copy.start()
    copy.wait()


def kernel(
    n_tile,
    n_col,
    adj_h,
    cen_h,
    side_h,
    vert_h,
    mask_h,
    mis_h,
    cell_h,
    cnt_s,
    fp_s,
    ff_s,
    out_ref,
    adj,
    cen,
    side,
    vert,
    mask,
    cell,
    plane,
    slots,
    rows_1h,
    vals_1h,
    acc,
    y_ref,
    r_ref,
    fixed_row,
    fixed_col,
    fixed_row_in,
    fixed_col_in,
    row_out,
    row_in,
    col_out,
    col_in,
    corner_out,
    corner_in,
    fold_out,
    line_bufs,
    pick_bufs,
    group_bufs,
    top_1h,
    delta,
    delta_out,
    delta_in,
    load_sem,
    plane_send,
    plane_recv,
    slot_send,
    slot_recv,
    fixed_send,
    fixed_recv,
    halo_send,
    halo_recv,
    line_send,
    line_recv,
    pick_send,
    pick_recv,
    delta_send,
    delta_recv,
):
    nx, nz, nc = grid_of(n_col)
    ng = nx * nc
    f32 = jnp.float32
    zero = f32(0)
    me = lax.axis_index("col")
    t = lax.axis_index("tile")
    core = me % nc
    my_z = (me // nc) % nz
    my_x = me // (nc * nz)
    my_g = my_x * nc + core
    sides = ((me + 1) % n_col, (me + n_col - 1) % n_col)
    tiles = (t + 1, t - 1)
    can_go = (t < n_tile - 1, t > 0)
    can_come = (t > 0, t < n_tile - 1)
    at_top = t == n_tile - 1

    def in_plane(g):
        return (g // nc) * nc * nz + my_z * nc + g % nc

    def on_line(z):
        return my_x * nc * nz + z * nc + core

    loads = [
        pltpu.make_async_copy(src, dst, load_sem.at[i])
        for i, (src, dst) in enumerate(
            [
                (mis_h.at[my_x, :, core], plane.at[my_g]),
                (side_h, side),
                (mask_h, mask),
                (cell_h, cell),
                (adj_h, adj),
                (cen_h, cen),
                (vert_h, vert),
            ]
        )
    ]
    for load in loads:
        load.start()

    for way, outermost in ((0, t < 1), (1, t > n_tile - 2)):

        @pl.when(outermost)
        def _():
            fixed_row_in[way][...] = jnp.zeros((LEVELS, COLS), f32)
            row_in[way][...] = jnp.zeros((2, LEVELS, COLS), f32)
            for across in range(2):
                corner_in[2 * way + across][...] = jnp.zeros((8, COLS), f32)

    barrier = pltpu.get_barrier_semaphore()

    def greet(where):
        pl.semaphore_signal(barrier, inc=1, device_id=where, device_id_type=MESH)

    @pl.loop(1, nz)
    def _(i):
        greet({"col": on_line((my_z + i) % nz)})

    @pl.loop(1, ng)
    def _(i):
        greet({"col": in_plane((my_g + i) % ng)})

    for side_id in sides:
        greet({"col": side_id})
    for way in range(2):

        @pl.when(can_go[way])
        def _():
            greet({"tile": tiles[way]})
            for side_id in sides:
                greet({"tile": tiles[way], "col": side_id})

    pl.semaphore_wait(
        barrier,
        nz - 1 + ng - 1 + 2 + 3 * (jnp.where(t > 0, 1, 0) + jnp.where(t < n_tile - 1, 1, 0)),
    )

    far_way = 1 - 2 * (my_z // (nz // 2))

    @pl.loop(1, ng)
    def _(i):
        g = (my_g + i) % ng
        copy_to(
            mis_h.at[g // nc, :, g % nc],
            plane.at[my_g],
            plane_send,
            plane_recv,
            {"col": in_plane(g)},
        ).start()

    def find(s, found):
        target = fp_s[s]
        return tuple(jnp.where(target == in_plane(g), s, found[g]) for g in range(ng)) + (
            jnp.where(target == me, s, found[ng]),
        )

    sources = lax.fori_loop(0, n_col, find, (jnp.int32(0),) * (ng + 1))
    my_source = sources[ng]
    flipped = ff_s[my_source]

    lanes = lax.broadcasted_iota(jnp.int32, (LEVELS, ROWS, COLS), 2)
    rows = lax.broadcasted_iota(jnp.int32, (LEVELS, ROWS, COLS), 1)
    q_lane = lax.broadcasted_iota(jnp.int32, (VREGS, 8, COLS), 2)
    q_id = lax.broadcasted_iota(jnp.int32, (VREGS, 8, COLS), 0)
    flat_lane = lax.broadcasted_iota(jnp.int32, (LEVELS, COLS), 1)
    flat_level = lax.broadcasted_iota(jnp.int32, (LEVELS, COLS), 0)
    tile_row = lax.broadcasted_iota(jnp.int32, (8, COLS), 0)
    edge_lane = (COLS - 1, 0)
    land_lane = (0, COLS - 1)
    edge_row = (ROWS - 1, 0)
    land_row = (0, ROWS - 1)

    def pack(cube, lane):
        edge = cube.reshape(VREGS, 8, COLS)[:, :, lane : lane + 1]
        return jnp.sum(jnp.where(q_lane == q_id, edge, zero), axis=0)

    def unpack(tile):
        spread = jnp.where(q_lane == q_id, tile[None], zero)
        return jnp.sum(spread, axis=2, keepdims=True).reshape(LEVELS, ROWS, 1)

    loads[1].wait()
    loads[2].wait()
    ocean = mask[...].astype(f32)
    for way in range(2):
        fixed_col[way][...] = pack(side[way] * ocean, edge_lane[way])
        fixed_row[way][...] = side[2 + way, :, edge_row[way], :] * mask[
            :, edge_row[way], :
        ].astype(f32)
    fixed = [
        copy_to(
            fixed_col[way],
            fixed_col_in[way],
            fixed_send.at[way],
            fixed_recv.at[way],
            {"col": sides[way]},
        )
        for way in range(2)
    ] + [
        copy_to(
            fixed_row[way],
            fixed_row_in[way],
            fixed_send.at[2 + way],
            fixed_recv.at[2 + way],
            {"tile": tiles[way]},
        )
        for way in range(2)
    ]
    for way in range(2):
        fixed[way].start()
        pl.when(can_go[way])(fixed[2 + way].start)

    loads[3].wait()
    row_ids = lax.broadcasted_iota(jnp.int32, (CELL_ROWS, COLS), 0)

    def columns_of(k, g):
        return pl.ds((k * ng + g) * COLS, COLS)

    order = nearest_first(my_z, nz)
    for k in range(nz):
        for g in range(ng):
            hit = row_ids == (cell[g // nc, order[k], g % nc] >> 7)
            rows_1h[:, columns_of(k, g)] = jnp.where(hit, f32(1), zero).astype(jnp.bfloat16)

    loads[0].wait()
    wait_for(plane.at[pl.ds(0, ng - 1)], plane_recv)

    for mine in range(nz):

        @pl.when(my_z == mine)
        def _():
            for z in sorted(range(nz), key=lambda z: -abs(z - mine))[:-1]:
                k = nearest_first(z, nz).index(mine)
                copy_to(
                    plane.at[:, z],
                    slots[k],
                    slot_send.at[z],
                    slot_recv.at[k],
                    {"col": on_line(z)},
                ).start()
            slots[0][...] = plane[:, mine]

    lane_ids = lax.broadcasted_iota(jnp.int32, (COLS, COLS), 0)
    slot_ids = lax.broadcasted_iota(jnp.int32, (1, COLS), 1)

    def fold_start(n, h):
        part = 2 * n + h
        line_bufs[part][my_z] = fold_out[part][...]

        @pl.loop(1, nz)
        def _(i):
            z = (my_z + nz + far_way * (nz - i)) % nz
            copy_to(
                fold_out[part],
                line_bufs[part].at[my_z],
                line_send.at[part],
                line_recv.at[part],
                {"col": on_line(z)},
            ).start()

    def fold_pick(n, h):
        part = 2 * n + h
        wait_for(line_bufs[part].at[pl.ds(0, nz - 1)], line_recv.at[part])
        for g in range(ng):
            pick_bufs[part][g] = line_bufs[part][(sources[g] // nc) % nz]

        @pl.loop(1, ng)
        def _(i):
            g = (my_g + i) % ng
            copy_to(
                pick_bufs[part].at[g],
                group_bufs[part].at[my_g],
                pick_send.at[part],
                pick_recv.at[part],
                {"col": in_plane(g)},
            ).start()

        group_bufs[part][my_g] = pick_bufs[part][my_g]

    def fold_finish(n, h):
        part = 2 * n + h
        count = PARTS[h][1] - PARTS[h][0]
        wait_for(group_bufs[part].at[pl.ds(0, ng - 1)], pick_recv.at[part])
        arrived = group_bufs[part][(my_source // (nc * nz)) * nc + my_source % nc]
        backwards = COLS - 1 - lax.broadcasted_iota(jnp.int32, (count, COLS), 1)
        turned = jnp.take_along_axis(arrived, backwards, axis=1)
        return jnp.where(flipped == 1, turned, arrived)

    for load in loads[4:]:
        load.wait()

    for k in range(nz):
        z, last = order[k], k == nz - 1
        if k:
            wait_for(slots[k], slot_recv.at[k])

        for g in range(ng):
            count = cnt_s[(g // nc) * nc * nz + z * nc + g % nc]
            value = jnp.where(slot_ids < count, slots[k][g], zero)
            high = value.astype(jnp.bfloat16).astype(f32)
            hit = lane_ids == (cell[g // nc, z, g % nc] & 127)
            for half, part in enumerate((high, value - high)):
                vals_1h[half * COLS : (half + 1) * COLS, g * COLS : (g + 1) * COLS] = jnp.where(
                    hit, part, zero
                ).astype(jnp.bfloat16)

        def lead():
            level_ids = lax.broadcasted_iota(jnp.int32, (ROWS, COLS), 0)
            for g in range(ng):
                cell_row = cell[g // nc, z, g % nc] >> 7
                level = jnp.where((cell_row & (ROWS - 1)) == ROWS - 1, cell_row >> 5, -1)
                top_1h[:, g * COLS : (g + 1) * COLS] = jnp.where(
                    level_ids == level, f32(1), zero
                ).astype(jnp.bfloat16)
            row = lax.dot_general(
                top_1h[...],
                vals_1h[...],
                (((1,), (1,)), ((), ())),
                preferred_element_type=f32,
            )[:LEVELS]
            row = row + acc[...].reshape(LEVELS, ROWS, 2 * COLS)[:, ROWS - 1, :]
            row = adj[:, ROWS - 1, :] + row[:, :COLS] + row[:, COLS:]
            for h, (low, high) in enumerate(PARTS):
                fold_out[h][...] = side[2, low:high, ROWS - 1, :] * row[low:high]
                fold_start(0, h)

        if last:
            pl.when(at_top)(lead)
        width = ng * COLS
        term = lax.dot_general(
            rows_1h[:, k * width : (k + 1) * width],
            vals_1h[...],
            (((1,), (1,)), ((), ())),
            preferred_element_type=f32,
        )
        if k:
            acc[...] += term
        else:
            acc[...] = term

    y_ref[...] = adj[...] + (acc[:, :COLS] + acc[:, COLS:]).reshape(LEVELS, ROWS, COLS)

    def interior(y):
        to_east = side[0] * y
        to_west = side[1] * y
        north = side[2] * y
        south = side[3] * y
        up = vert[0] * y
        down = vert[1] * y
        level = jnp.zeros((1, ROWS, COLS), f32)
        r = (
            cen[...] * y
            + jnp.where(lanes == 0, zero, pltpu.roll(to_east, 1, 2))
            + jnp.where(lanes == COLS - 1, zero, pltpu.roll(to_west, COLS - 1, 2))
            + jnp.where(rows == 0, zero, pltpu.roll(north, 1, 1))
            + jnp.where(rows == ROWS - 1, zero, pltpu.roll(south, ROWS - 1, 1))
            + jnp.concatenate([up[1:], level], axis=0)
            + jnp.concatenate([level, down[:-1]], axis=0)
        )
        return r

    r_ref[...] = interior(y_ref[...])
    for way in range(2):
        col_out[way][0] = pack(side[way] * y_ref[...], edge_lane[way])
        col_out[way][1] = fixed_col[way][...] * pack(r_ref[...], edge_lane[way])
        at = edge_row[way]
        row_out[way][0] = side[2 + way, :, at, :] * y_ref[:, at, :]
        row_out[way][1] = fixed_row[way][...] * r_ref[:, at, :]
        for across in range(2):
            lane = edge_lane[across]
            spot = flat_lane == 4 * flat_level + 3 * way
            level_value = y_ref[:, at, :][:, lane : lane + 1]
            for part, weight in enumerate((side[2 + way, :, at, :], side[across, :, at, :])):
                term = weight[:, lane : lane + 1] * level_value
                corner_out[2 * way + across][part : part + 1, :] = jnp.sum(
                    jnp.where(spot, term, zero), axis=0, keepdims=True
                )

    halos = []
    for way in range(2):
        halos.append(
            copy_to(
                col_out[way],
                col_in[way],
                halo_send.at[way],
                halo_recv.at[way],
                {"col": sides[way]},
            )
        )
        halos[-1].start()
    far = []
    for way in range(2):
        far.append(
            [
                copy_to(
                    row_out[way],
                    row_in[way],
                    halo_send.at[2 + way],
                    halo_recv.at[2 + way],
                    {"tile": tiles[way]},
                )
            ]
            + [
                copy_to(
                    corner_out[2 * way + across],
                    corner_in[2 * way + across],
                    halo_send.at[4 + 2 * way + across],
                    halo_recv.at[4 + 2 * way + across],
                    {"tile": tiles[way], "col": sides[across]},
                )
                for across in range(2)
            ]
        )

        @pl.when(can_go[way])
        def _():
            for copy in far[way]:
                copy.start()

    @pl.when(at_top)
    def _():
        for h in range(2):
            fold_pick(0, h)

    for way in range(2):
        halos[way].wait_recv()
        fixed[way].wait_recv()

        @pl.when(can_come[way])
        def _():
            fixed[2 + way].wait_recv()
            for copy in far[way]:
                copy.wait_recv()

    def with_sides(r, west, east):
        return r + jnp.where(lanes == 0, west, jnp.where(lanes == COLS - 1, east, zero))

    for way in range(2):
        at = land_row[way]
        r_ref[:, at, :] = r_ref[:, at, :] + row_in[way][0]
    y_ref[...] = with_sides(r_ref[...], unpack(col_in[0][0]), unpack(col_in[1][0])) * mask[
        ...
    ].astype(f32)

    top = ROWS - 1
    moves = [
        copy_to(
            delta_out[way],
            delta_in[way],
            delta_send.at[way],
            delta_recv.at[way],
            {"col": sides[way]},
        )
        for way in range(2)
    ]

    @pl.when(at_top)
    def _():
        for h, (low, high) in enumerate(PARTS):
            edge = mask[low:high, top, :].astype(f32) * fold_finish(0, h)
            delta[low:high, :] = edge
            fold_out[2 + h][...] = side[2, low:high, top, :] * (y_ref[low:high, top, :] + edge)
            fold_start(1, h)
        for way in range(2):
            delta_out[way][...] = side[way, :, top, :] * delta[...]
            moves[way].start()

    ring = []
    for across in range(2):
        lacked = col_out[1 - across][0]
        for way, sub in ((0, 0), (1, 7)):
            lacked = lacked + jnp.where(tile_row == sub, corner_in[2 * way + across][0:1, :], zero)
        ring.append(col_in[across][1] + fixed_col_in[across][...] * lacked)
    r_ref[...] = with_sides(interior(y_ref[...]), unpack(ring[0]), unpack(ring[1]))
    for way in range(2):
        lacked = row_out[1 - way][0]
        for across in range(2):
            spot = flat_lane == 4 * flat_level + 3 * way
            term = jnp.sum(
                jnp.where(spot, corner_in[2 * way + across][1:2, :], zero), axis=1, keepdims=True
            )
            lacked = lacked + jnp.where(flat_lane == land_lane[across], term, zero)
        at = land_row[way]
        r_ref[:, at, :] = r_ref[:, at, :] + (row_in[way][1] + fixed_row_in[way][...] * lacked)
    out_ref[...] = r_ref[...] * mask[...].astype(f32)

    @pl.when(at_top)
    def _():
        level = jnp.zeros((1, COLS), f32)
        up = vert[0, :, top, :] * delta[...]
        down = vert[1, :, top, :] * delta[...]
        change = (
            cen[:, top, :] * delta[...]
            + jnp.concatenate([up[1:], level], axis=0)
            + jnp.concatenate([level, down[:-1]], axis=0)
        )
        for way in range(2):
            moves[way].wait_recv()
            shift = 1 if way == 0 else COLS - 1
            change = change + jnp.where(
                flat_lane == land_lane[way],
                pltpu.roll(delta_in[way][...], shift, 1),
                pltpu.roll(delta_out[way][...], shift, 1),
            )
        below = side[3, :, top, :] * delta[...]
        out_ref[:, top - 1, :] = out_ref[:, top - 1, :] + below * mask[:, top - 1, :].astype(f32)
        delta[...] = change
        for h in range(2):
            fold_pick(1, h)
        for h, (low, high) in enumerate(PARTS):
            total = delta[low:high, :] + fold_finish(1, h)
            out_ref[low:high, top, :] = out_ref[low:high, top, :] + total * mask[
                low:high, top, :
            ].astype(f32)
        for way in range(2):
            moves[way].wait_send()
        for part in range(4):
            wait_for(line_bufs[part].at[pl.ds(0, nz - 1)], line_send.at[part])
            wait_for(group_bufs[part].at[pl.ds(0, ng - 1)], pick_send.at[part])

    wait_for(plane.at[pl.ds(0, ng - 1)], plane_send)

    @pl.loop(1, nz)
    def _(i):
        wait_for(slots[0], slot_send.at[(my_z + i) % nz])

    for way in range(2):
        halos[way].wait_send()
        fixed[way].wait_send()

        @pl.when(can_go[way])
        def _():
            fixed[2 + way].wait_send()
            for copy in far[way]:
                copy.wait_send()


def solution(mesh):
    n_tile, n_col = mesh.shape["tile"], mesh.shape["col"]
    nx, nz, nc = grid_of(n_col)
    ng = nx * nc
    cube = (LEVELS, ROWS, COLS)
    flat = (LEVELS, COLS)
    parts = [(high - low, COLS) for low, high in PARTS] * 2
    f32 = jnp.float32
    any_space = pl.BlockSpec(memory_space=pl.ANY)
    scalars = pl.BlockSpec(memory_space=pltpu.SMEM)
    dma = pltpu.SemaphoreType.DMA

    def body(adj, cen, side, vert, mask, misfit, cell, count, partner, flip):
        result = pl.pallas_call(
            functools.partial(kernel, n_tile, n_col),
            out_shape=pltpu.VMEM(cube, f32),
            in_specs=[any_space] * 7 + [scalars] * 3,
            out_specs=pl.BlockSpec(memory_space=pltpu.VMEM),
            scratch_shapes=[
                pltpu.VMEM(cube, f32),
                pltpu.VMEM(cube, f32),
                pltpu.VMEM((4,) + cube, f32),
                pltpu.VMEM((2,) + cube, f32),
                pltpu.VMEM(cube, jnp.int32),
                pltpu.VMEM((nx, nz, nc, 1, COLS), jnp.int32),
                pltpu.VMEM((ng, nz, 1, COLS), f32),
                [pltpu.VMEM((ng, 1, COLS), f32)] * nz,
                pltpu.VMEM((CELL_ROWS, n_col * COLS), jnp.bfloat16),
                pltpu.VMEM((2 * COLS, ng * COLS), jnp.bfloat16),
                pltpu.VMEM((CELL_ROWS, 2 * COLS), f32),
                pltpu.VMEM(cube, f32),
                pltpu.VMEM(cube, f32),
                [pltpu.VMEM(flat, f32)] * 2,
                [pltpu.VMEM((8, COLS), f32)] * 2,
                [pltpu.VMEM(flat, f32)] * 2,
                [pltpu.VMEM((8, COLS), f32)] * 2,
                [pltpu.VMEM((2,) + flat, f32)] * 2,
                [pltpu.VMEM((2,) + flat, f32)] * 2,
                [pltpu.VMEM((2, 8, COLS), f32)] * 2,
                [pltpu.VMEM((2, 8, COLS), f32)] * 2,
                [pltpu.VMEM((8, COLS), f32)] * 4,
                [pltpu.VMEM((8, COLS), f32)] * 4,
                [pltpu.VMEM(part, f32) for part in parts],
                [pltpu.VMEM((nz,) + part, f32) for part in parts],
                [pltpu.VMEM((ng,) + part, f32) for part in parts],
                [pltpu.VMEM((ng,) + part, f32) for part in parts],
                pltpu.VMEM((ROWS, ng * COLS), jnp.bfloat16),
                pltpu.VMEM(flat, f32),
                [pltpu.VMEM(flat, f32)] * 2,
                [pltpu.VMEM(flat, f32)] * 2,
                dma((7,)),
                dma,
                dma,
                dma((nz,)),
                dma((nz,)),
                dma((4,)),
                dma((4,)),
                dma((8,)),
                dma((8,)),
                dma((4,)),
                dma((4,)),
                dma((4,)),
                dma((4,)),
                dma((2,)),
                dma((2,)),
            ],
            compiler_params=pltpu.CompilerParams(
                collective_id=0, has_side_effects=True, vmem_limit_bytes=60 * 2**20
            ),
        )(
            adj,
            cen,
            side,
            vert,
            mask,
            misfit.reshape(nx, nz, nc, 1, COLS),
            cell.reshape(nx, nz, nc, 1, COLS),
            count.reshape(n_col),
            partner,
            flip,
        )
        return pl.pallas_call(
            hand_out,
            out_shape=jax.ShapeDtypeStruct(cube, f32),
            in_specs=[pl.BlockSpec(memory_space=pltpu.VMEM)],
            out_specs=any_space,
            scratch_shapes=[dma],
            compiler_params=pltpu.CompilerParams(vmem_limit_bytes=2**20),
        )(result)

    in_specs = (
        P(None, "tile", "col"),
        P(None, "tile", "col"),
        P(None, None, "tile", "col"),
        P(None, None, "tile", "col"),
        P(None, "tile", "col"),
        P("tile", "col", None, None),
        P("tile", "col", None, None),
        P("tile", "col", None),
        P(),
        P(),
    )
    out_specs = P(None, "tile", "col")
    return jax.shard_map(body, mesh=mesh, in_specs=in_specs, out_specs=out_specs, check_vma=False)
```

```python
import functools

import jax
import jax.numpy as jnp
from jax import lax
from jax.experimental import pallas as pl
from jax.experimental.pallas import tpu as pltpu
from jax.sharding import PartitionSpec as P

LEVELS = 25
ROWS = 32
COLS = 128
CELL_ROWS = LEVELS * ROWS
VREGS = CELL_ROWS // 8
PARTS = ((0, 16), (16, LEVELS))
MESH = pl.DeviceIdType.MESH


def grid_of(n_col):
    return (4, 6, 2) if n_col == 48 else (2, n_col // 4, 2)


def nearest_first(z, nz):
    short = z * (nz - 1 - z) // 3
    longer = 1 - 2 * (z // (nz // 2))
    order = []
    for k in range(nz):
        both = (k + 1) // 2 * (1 if k % 2 else -1)
        two_sided = (2 * short - k + nz) // nz
        order.append(z + longer * (two_sided * both + (1 - two_sided) * (k - short)))
    return order


def copy_to(src, dst, send, recv, where):
    return pltpu.make_async_remote_copy(
        src_ref=src,
        dst_ref=dst,
        send_sem=send,
        recv_sem=recv,
        device_id=where,
        device_id_type=MESH,
    )


def wait_for(ref, sem):
    pltpu.make_async_copy(ref, ref, sem).wait()


def hand_out(result, out_h, sem):
    copy = pltpu.make_async_copy(result, out_h, sem)
    copy.start()
    copy.wait()


def kernel(
    n_tile,
    n_col,
    adj_h,
    cen_h,
    side_h,
    vert_h,
    mask_h,
    mis_h,
    cell_h,
    cnt_s,
    fp_s,
    ff_s,
    out_ref,
    adj,
    cen,
    side,
    vert,
    mask,
    cell,
    plane,
    slots,
    rows_1h,
    vals_1h,
    acc,
    y_ref,
    r_ref,
    fixed_row,
    fixed_col,
    fixed_row_in,
    fixed_col_in,
    row_out,
    row_in,
    col_out,
    col_in,
    corner_out,
    corner_in,
    fold_out,
    line_bufs,
    pick_bufs,
    group_bufs,
    top_1h,
    delta,
    delta_out,
    delta_in,
    load_sem,
    plane_send,
    plane_recv,
    slot_send,
    slot_recv,
    fixed_send,
    fixed_recv,
    halo_send,
    halo_recv,
    line_send,
    line_recv,
    pick_send,
    pick_recv,
    delta_send,
    delta_recv,
):
    nx, nz, nc = grid_of(n_col)
    ng = nx * nc
    f32 = jnp.float32
    zero = f32(0)
    me = lax.axis_index("col")
    t = lax.axis_index("tile")
    core = me % nc
    my_z = (me // nc) % nz
    my_x = me // (nc * nz)
    my_g = my_x * nc + core
    sides = ((me + 1) % n_col, (me + n_col - 1) % n_col)
    tiles = (t + 1, t - 1)
    can_go = (t < n_tile - 1, t > 0)
    can_come = (t > 0, t < n_tile - 1)
    at_top = t == n_tile - 1

    def in_plane(g):
        return (g // nc) * nc * nz + my_z * nc + g % nc

    def on_line(z):
        return my_x * nc * nz + z * nc + core

    loads = [
        pltpu.make_async_copy(src, dst, load_sem.at[i])
        for i, (src, dst) in enumerate(
            [
                (mis_h.at[my_x, :, core], plane.at[my_g]),
                (side_h, side),
                (mask_h, mask),
                (cell_h, cell),
                (adj_h, adj),
                (cen_h, cen),
                (vert_h, vert),
            ]
        )
    ]
    for load in loads:
        load.start()

    for way, outermost in ((0, t < 1), (1, t > n_tile - 2)):

        @pl.when(outermost)
        def _():
            fixed_row_in[way][...] = jnp.zeros((LEVELS, COLS), f32)
            row_in[way][...] = jnp.zeros((2, LEVELS, COLS), f32)
            for across in range(2):
                corner_in[2 * way + across][...] = jnp.zeros((8, COLS), f32)

    barrier = pltpu.get_barrier_semaphore()

    def greet(where):
        pl.semaphore_signal(barrier, inc=1, device_id=where, device_id_type=MESH)

    @pl.loop(1, nz)
    def _(i):
        greet({"col": on_line((my_z + i) % nz)})

    @pl.loop(1, ng)
    def _(i):
        greet({"col": in_plane((my_g + i) % ng)})

    for side_id in sides:
        greet({"col": side_id})
    for way in range(2):

        @pl.when(can_go[way])
        def _():
            greet({"tile": tiles[way]})
            for side_id in sides:
                greet({"tile": tiles[way], "col": side_id})

    pl.semaphore_wait(
        barrier,
        nz - 1 + ng - 1 + 2 + 3 * (jnp.where(t > 0, 1, 0) + jnp.where(t < n_tile - 1, 1, 0)),
    )

    far_way = 1 - 2 * (my_z // (nz // 2))

    @pl.loop(1, ng)
    def _(i):
        g = (my_g + i) % ng
        copy_to(
            mis_h.at[g // nc, :, g % nc],
            plane.at[my_g],
            plane_send,
            plane_recv,
            {"col": in_plane(g)},
        ).start()

    def find(s, found):
        target = fp_s[s]
        return tuple(jnp.where(target == in_plane(g), s, found[g]) for g in range(ng)) + (
            jnp.where(target == me, s, found[ng]),
        )

    sources = lax.fori_loop(0, n_col, find, (jnp.int32(0),) * (ng + 1))
    my_source = sources[ng]

    def find_again(s, found):
        target = fp_s[s]
        return tuple(jnp.where(target == sources[g], s, found[g]) for g in range(ng + 1))

    sources_2 = lax.fori_loop(0, n_col, find_again, (jnp.int32(0),) * (ng + 1))
    my_source_2 = sources_2[ng]

    lanes = lax.broadcasted_iota(jnp.int32, (LEVELS, ROWS, COLS), 2)
    rows = lax.broadcasted_iota(jnp.int32, (LEVELS, ROWS, COLS), 1)
    q_lane = lax.broadcasted_iota(jnp.int32, (VREGS, 8, COLS), 2)
    q_id = lax.broadcasted_iota(jnp.int32, (VREGS, 8, COLS), 0)
    flat_lane = lax.broadcasted_iota(jnp.int32, (LEVELS, COLS), 1)
    flat_level = lax.broadcasted_iota(jnp.int32, (LEVELS, COLS), 0)
    tile_row = lax.broadcasted_iota(jnp.int32, (8, COLS), 0)
    edge_lane = (COLS - 1, 0)
    land_lane = (0, COLS - 1)
    edge_row = (ROWS - 1, 0)
    land_row = (0, ROWS - 1)

    def pack(cube, lane):
        edge = cube.reshape(VREGS, 8, COLS)[:, :, lane : lane + 1]
        return jnp.sum(jnp.where(q_lane == q_id, edge, zero), axis=0)

    def unpack(tile):
        spread = jnp.where(q_lane == q_id, tile[None], zero)
        return jnp.sum(spread, axis=2, keepdims=True).reshape(LEVELS, ROWS, 1)

    def fold_start(n, h):
        part = 2 * n + h
        line_bufs[part][my_z] = fold_out[part][...]

        @pl.loop(1, nz)
        def _(i):
            z = (my_z + nz + far_way * (nz - i)) % nz
            copy_to(
                fold_out[part],
                line_bufs[part].at[my_z],
                line_send.at[part],
                line_recv.at[part],
                {"col": on_line(z)},
            ).start()

    def fold_wait(n, h):
        part = 2 * n + h
        wait_for(line_bufs[part].at[pl.ds(0, nz - 1)], line_recv.at[part])

    def fold_pick(n, h, chosen, to):
        part, end = 2 * n + h, 2 * to + h
        for g in range(ng):
            pick_bufs[end][g] = line_bufs[part][(chosen[g] // nc) % nz]

        @pl.loop(1, ng)
        def _(i):
            g = (my_g + i) % ng
            copy_to(
                pick_bufs[end].at[g],
                group_bufs[end].at[my_g],
                pick_send.at[end],
                pick_recv.at[end],
                {"col": in_plane(g)},
            ).start()

        group_bufs[end][my_g] = pick_bufs[end][my_g]

    def fold_finish(n, h, source, turns):
        end = 2 * n + h
        count = PARTS[h][1] - PARTS[h][0]
        wait_for(group_bufs[end].at[pl.ds(0, ng - 1)], pick_recv.at[end])
        arrived = group_bufs[end][(source // (nc * nz)) * nc + source % nc]
        backwards = COLS - 1 - lax.broadcasted_iota(jnp.int32, (count, COLS), 1)
        for column in turns:
            turned = jnp.take_along_axis(arrived, backwards, axis=1)
            arrived = jnp.where(ff_s[column] == 1, turned, arrived)
        return arrived

    loads[1].wait()
    loads[2].wait()
    ocean = mask[...].astype(f32)
    for way in range(2):
        fixed_col[way][...] = pack(side[way] * ocean, edge_lane[way])
        fixed_row[way][...] = side[2 + way, :, edge_row[way], :] * mask[
            :, edge_row[way], :
        ].astype(f32)
    fixed = [
        copy_to(
            fixed_col[way],
            fixed_col_in[way],
            fixed_send.at[way],
            fixed_recv.at[way],
            {"col": sides[way]},
        )
        for way in range(2)
    ] + [
        copy_to(
            fixed_row[way],
            fixed_row_in[way],
            fixed_send.at[2 + way],
            fixed_recv.at[2 + way],
            {"tile": tiles[way]},
        )
        for way in range(2)
    ]
    @pl.when(at_top)
    def _():
        for h, (low, high) in enumerate(PARTS):
            fold_out[4 + h][...] = fixed_row[0][low:high, :]
            fold_start(2, h)

    for way in range(2):
        fixed[way].start()
        pl.when(can_go[way])(fixed[2 + way].start)

    loads[3].wait()
    row_ids = lax.broadcasted_iota(jnp.int32, (CELL_ROWS, COLS), 0)

    def columns_of(k, g):
        return pl.ds((k * ng + g) * COLS, COLS)

    order = nearest_first(my_z, nz)
    for k in range(nz):
        for g in range(ng):
            hit = row_ids == (cell[g // nc, order[k], g % nc] >> 7)
            rows_1h[:, columns_of(k, g)] = jnp.where(hit, f32(1), zero).astype(jnp.bfloat16)

    loads[0].wait()
    wait_for(plane.at[pl.ds(0, ng - 1)], plane_recv)

    for mine in range(nz):

        @pl.when(my_z == mine)
        def _():
            for z in sorted(range(nz), key=lambda z: -abs(z - mine))[:-1]:
                k = nearest_first(z, nz).index(mine)
                copy_to(
                    plane.at[:, z],
                    slots[k],
                    slot_send.at[z],
                    slot_recv.at[k],
                    {"col": on_line(z)},
                ).start()
            slots[0][...] = plane[:, mine]

    lane_ids = lax.broadcasted_iota(jnp.int32, (COLS, COLS), 0)
    slot_ids = lax.broadcasted_iota(jnp.int32, (1, COLS), 1)

    for load in loads[4:]:
        load.wait()

    for k in range(nz):
        z, last = order[k], k == nz - 1
        if k:
            wait_for(slots[k], slot_recv.at[k])

        for g in range(ng):
            count = cnt_s[(g // nc) * nc * nz + z * nc + g % nc]
            value = jnp.where(slot_ids < count, slots[k][g], zero)
            high = value.astype(jnp.bfloat16).astype(f32)
            hit = lane_ids == (cell[g // nc, z, g % nc] & 127)
            for half, part in enumerate((high, value - high)):
                vals_1h[half * COLS : (half + 1) * COLS, g * COLS : (g + 1) * COLS] = jnp.where(
                    hit, part, zero
                ).astype(jnp.bfloat16)

        def lead():
            level_ids = lax.broadcasted_iota(jnp.int32, (ROWS, COLS), 0)
            for g in range(ng):
                cell_row = cell[g // nc, z, g % nc] >> 7
                level = jnp.where((cell_row & (ROWS - 1)) == ROWS - 1, cell_row >> 5, -1)
                top_1h[:, g * COLS : (g + 1) * COLS] = jnp.where(
                    level_ids == level, f32(1), zero
                ).astype(jnp.bfloat16)
            row = lax.dot_general(
                top_1h[...],
                vals_1h[...],
                (((1,), (1,)), ((), ())),
                preferred_element_type=f32,
            )[:LEVELS]
            row = row + acc[...].reshape(LEVELS, ROWS, 2 * COLS)[:, ROWS - 1, :]
            row = adj[:, ROWS - 1, :] + row[:, :COLS] + row[:, COLS:]
            for h, (low, high) in enumerate(PARTS):
                fold_out[h][...] = side[2, low:high, ROWS - 1, :] * row[low:high]
                fold_start(0, h)

        if last:
            pl.when(at_top)(lead)
        width = ng * COLS
        term = lax.dot_general(
            rows_1h[:, k * width : (k + 1) * width],
            vals_1h[...],
            (((1,), (1,)), ((), ())),
            preferred_element_type=f32,
        )
        if k:
            acc[...] += term
        else:
            acc[...] = term

    y_ref[...] = adj[...] + (acc[:, :COLS] + acc[:, COLS:]).reshape(LEVELS, ROWS, COLS)

    def interior(y):
        to_east = side[0] * y
        to_west = side[1] * y
        north = side[2] * y
        south = side[3] * y
        up = vert[0] * y
        down = vert[1] * y
        level = jnp.zeros((1, ROWS, COLS), f32)
        r = (
            cen[...] * y
            + jnp.where(lanes == 0, zero, pltpu.roll(to_east, 1, 2))
            + jnp.where(lanes == COLS - 1, zero, pltpu.roll(to_west, COLS - 1, 2))
            + jnp.where(rows == 0, zero, pltpu.roll(north, 1, 1))
            + jnp.where(rows == ROWS - 1, zero, pltpu.roll(south, ROWS - 1, 1))
            + jnp.concatenate([up[1:], level], axis=0)
            + jnp.concatenate([level, down[:-1]], axis=0)
        )
        return r

    r_ref[...] = interior(y_ref[...])
    for way in range(2):
        col_out[way][0] = pack(side[way] * y_ref[...], edge_lane[way])
        col_out[way][1] = fixed_col[way][...] * pack(r_ref[...], edge_lane[way])
        at = edge_row[way]
        row_out[way][0] = side[2 + way, :, at, :] * y_ref[:, at, :]
        row_out[way][1] = fixed_row[way][...] * r_ref[:, at, :]
        for across in range(2):
            lane = edge_lane[across]
            spot = flat_lane == 4 * flat_level + 3 * way
            level_value = y_ref[:, at, :][:, lane : lane + 1]
            for part, weight in enumerate((side[2 + way, :, at, :], side[across, :, at, :])):
                term = weight[:, lane : lane + 1] * level_value
                corner_out[2 * way + across][part : part + 1, :] = jnp.sum(
                    jnp.where(spot, term, zero), axis=0, keepdims=True
                )

    halos = []
    for way in range(2):
        halos.append(
            copy_to(
                col_out[way],
                col_in[way],
                halo_send.at[way],
                halo_recv.at[way],
                {"col": sides[way]},
            )
        )
        halos[-1].start()
    far = []
    for way in range(2):
        far.append(
            [
                copy_to(
                    row_out[way],
                    row_in[way],
                    halo_send.at[2 + way],
                    halo_recv.at[2 + way],
                    {"tile": tiles[way]},
                )
            ]
            + [
                copy_to(
                    corner_out[2 * way + across],
                    corner_in[2 * way + across],
                    halo_send.at[4 + 2 * way + across],
                    halo_recv.at[4 + 2 * way + across],
                    {"tile": tiles[way], "col": sides[across]},
                )
                for across in range(2)
            ]
        )

        @pl.when(can_go[way])
        def _():
            for copy in far[way]:
                copy.start()

    @pl.when(at_top)
    def _():
        for h in range(2):
            fold_wait(2, h)
            fold_pick(2, h, sources, 2)
        for h in range(2):
            fold_wait(0, h)
            fold_pick(0, h, sources, 0)
        for h in range(2):
            fold_pick(0, h, sources_2, 3)

    for way in range(2):
        halos[way].wait_recv()
        fixed[way].wait_recv()

        @pl.when(can_come[way])
        def _():
            fixed[2 + way].wait_recv()
            for copy in far[way]:
                copy.wait_recv()

    def with_sides(r, west, east):
        return r + jnp.where(lanes == 0, west, jnp.where(lanes == COLS - 1, east, zero))

    for way in range(2):
        at = land_row[way]
        r_ref[:, at, :] = r_ref[:, at, :] + row_in[way][0]
    y_ref[...] = with_sides(r_ref[...], unpack(col_in[0][0]), unpack(col_in[1][0])) * mask[
        ...
    ].astype(f32)

    top = ROWS - 1
    moves = [
        copy_to(
            delta_out[way],
            delta_in[way],
            delta_send.at[way],
            delta_recv.at[way],
            {"col": sides[way]},
        )
        for way in range(2)
    ]

    @pl.when(at_top)
    def _():
        for h, (low, high) in enumerate(PARTS):
            fold_out[2 + h][...] = side[2, low:high, top, :] * y_ref[low:high, top, :]
            fold_start(1, h)
        for h, (low, high) in enumerate(PARTS):
            delta[low:high, :] = mask[low:high, top, :].astype(f32) * fold_finish(
                0, h, my_source, [my_source]
            )
        for way in range(2):
            delta_out[way][...] = side[way, :, top, :] * delta[...]
            moves[way].start()

    ring = []
    for across in range(2):
        lacked = col_out[1 - across][0]
        for way, sub in ((0, 0), (1, 7)):
            lacked = lacked + jnp.where(tile_row == sub, corner_in[2 * way + across][0:1, :], zero)
        ring.append(col_in[across][1] + fixed_col_in[across][...] * lacked)
    r_ref[...] = with_sides(interior(y_ref[...]), unpack(ring[0]), unpack(ring[1]))
    for way in range(2):
        lacked = row_out[1 - way][0]
        for across in range(2):
            spot = flat_lane == 4 * flat_level + 3 * way
            term = jnp.sum(
                jnp.where(spot, corner_in[2 * way + across][1:2, :], zero), axis=1, keepdims=True
            )
            lacked = lacked + jnp.where(flat_lane == land_lane[across], term, zero)
        at = land_row[way]
        r_ref[:, at, :] = r_ref[:, at, :] + (row_in[way][1] + fixed_row_in[way][...] * lacked)
    out_ref[...] = r_ref[...] * mask[...].astype(f32)

    @pl.when(at_top)
    def _():
        level = jnp.zeros((1, COLS), f32)
        up = vert[0, :, top, :] * delta[...]
        down = vert[1, :, top, :] * delta[...]
        change = (
            cen[:, top, :] * delta[...]
            + jnp.concatenate([up[1:], level], axis=0)
            + jnp.concatenate([level, down[:-1]], axis=0)
        )
        for way in range(2):
            moves[way].wait_recv()
            shift = 1 if way == 0 else COLS - 1
            change = change + jnp.where(
                flat_lane == land_lane[way],
                pltpu.roll(delta_in[way][...], shift, 1),
                pltpu.roll(delta_out[way][...], shift, 1),
            )
        below = side[3, :, top, :] * delta[...]
        out_ref[:, top - 1, :] = out_ref[:, top - 1, :] + below * mask[:, top - 1, :].astype(f32)
        delta[...] = change
        for h, (low, high) in enumerate(PARTS):
            delta[low:high, :] = delta[low:high, :] + fold_finish(
                2, h, my_source, [my_source]
            ) * fold_finish(3, h, my_source_2, [my_source_2, my_source])
        for h in range(2):
            fold_wait(1, h)
            fold_pick(1, h, sources, 1)
        for h, (low, high) in enumerate(PARTS):
            total = delta[low:high, :] + fold_finish(1, h, my_source, [my_source])
            out_ref[low:high, top, :] = out_ref[low:high, top, :] + total * mask[
                low:high, top, :
            ].astype(f32)
        for way in range(2):
            moves[way].wait_send()
        for part in range(6):
            wait_for(line_bufs[part].at[pl.ds(0, nz - 1)], line_send.at[part])
        for part in range(8):
            wait_for(group_bufs[part].at[pl.ds(0, ng - 1)], pick_send.at[part])

    wait_for(plane.at[pl.ds(0, ng - 1)], plane_send)

    @pl.loop(1, nz)
    def _(i):
        wait_for(slots[0], slot_send.at[(my_z + i) % nz])

    for way in range(2):
        halos[way].wait_send()
        fixed[way].wait_send()

        @pl.when(can_go[way])
        def _():
            fixed[2 + way].wait_send()
            for copy in far[way]:
                copy.wait_send()


def solution(mesh):
    n_tile, n_col = mesh.shape["tile"], mesh.shape["col"]
    nx, nz, nc = grid_of(n_col)
    ng = nx * nc
    cube = (LEVELS, ROWS, COLS)
    flat = (LEVELS, COLS)
    parts = [(high - low, COLS) for low, high in PARTS]
    f32 = jnp.float32
    any_space = pl.BlockSpec(memory_space=pl.ANY)
    scalars = pl.BlockSpec(memory_space=pltpu.SMEM)
    dma = pltpu.SemaphoreType.DMA

    def body(adj, cen, side, vert, mask, misfit, cell, count, partner, flip):
        result = pl.pallas_call(
            functools.partial(kernel, n_tile, n_col),
            out_shape=pltpu.VMEM(cube, f32),
            in_specs=[any_space] * 7 + [scalars] * 3,
            out_specs=pl.BlockSpec(memory_space=pltpu.VMEM),
            scratch_shapes=[
                pltpu.VMEM(cube, f32),
                pltpu.VMEM(cube, f32),
                pltpu.VMEM((4,) + cube, f32),
                pltpu.VMEM((2,) + cube, f32),
                pltpu.VMEM(cube, jnp.int32),
                pltpu.VMEM((nx, nz, nc, 1, COLS), jnp.int32),
                pltpu.VMEM((ng, nz, 1, COLS), f32),
                [pltpu.VMEM((ng, 1, COLS), f32)] * nz,
                pltpu.VMEM((CELL_ROWS, n_col * COLS), jnp.bfloat16),
                pltpu.VMEM((2 * COLS, ng * COLS), jnp.bfloat16),
                pltpu.VMEM((CELL_ROWS, 2 * COLS), f32),
                pltpu.VMEM(cube, f32),
                pltpu.VMEM(cube, f32),
                [pltpu.VMEM(flat, f32)] * 2,
                [pltpu.VMEM((8, COLS), f32)] * 2,
                [pltpu.VMEM(flat, f32)] * 2,
                [pltpu.VMEM((8, COLS), f32)] * 2,
                [pltpu.VMEM((2,) + flat, f32)] * 2,
                [pltpu.VMEM((2,) + flat, f32)] * 2,
                [pltpu.VMEM((2, 8, COLS), f32)] * 2,
                [pltpu.VMEM((2, 8, COLS), f32)] * 2,
                [pltpu.VMEM((8, COLS), f32)] * 4,
                [pltpu.VMEM((8, COLS), f32)] * 4,
                [pltpu.VMEM(part, f32) for part in parts * 3],
                [pltpu.VMEM((nz,) + part, f32) for part in parts * 3],
                [pltpu.VMEM((ng,) + part, f32) for part in parts * 4],
                [pltpu.VMEM((ng,) + part, f32) for part in parts * 4],
                pltpu.VMEM((ROWS, ng * COLS), jnp.bfloat16),
                pltpu.VMEM(flat, f32),
                [pltpu.VMEM(flat, f32)] * 2,
                [pltpu.VMEM(flat, f32)] * 2,
                dma((7,)),
                dma,
                dma,
                dma((nz,)),
                dma((nz,)),
                dma((4,)),
                dma((4,)),
                dma((8,)),
                dma((8,)),
                dma((6,)),
                dma((6,)),
                dma((8,)),
                dma((8,)),
                dma((2,)),
                dma((2,)),
            ],
            compiler_params=pltpu.CompilerParams(
                collective_id=0, has_side_effects=True, vmem_limit_bytes=60 * 2**20
            ),
        )(
            adj,
            cen,
            side,
            vert,
            mask,
            misfit.reshape(nx, nz, nc, 1, COLS),
            cell.reshape(nx, nz, nc, 1, COLS),
            count.reshape(n_col),
            partner,
            flip,
        )
        return pl.pallas_call(
            hand_out,
            out_shape=jax.ShapeDtypeStruct(cube, f32),
            in_specs=[pl.BlockSpec(memory_space=pltpu.VMEM)],
            out_specs=any_space,
            scratch_shapes=[dma],
            compiler_params=pltpu.CompilerParams(vmem_limit_bytes=2**20),
        )(result)

    in_specs = (
        P(None, "tile", "col"),
        P(None, "tile", "col"),
        P(None, None, "tile", "col"),
        P(None, None, "tile", "col"),
        P(None, "tile", "col"),
        P("tile", "col", None, None),
        P("tile", "col", None, None),
        P("tile", "col", None),
        P(),
        P(),
    )
    out_specs = P(None, "tile", "col")
    return jax.shard_map(body, mesh=mesh, in_specs=in_specs, out_specs=out_specs, check_vma=False)
```

```python
import functools

import jax
import jax.numpy as jnp
from jax import lax
from jax.experimental import pallas as pl
from jax.experimental.pallas import tpu as pltpu
from jax.sharding import PartitionSpec as P

LEVELS = 25
ROWS = 32
COLS = 128
CELL_ROWS = LEVELS * ROWS
VREGS = CELL_ROWS // 8
PARTS = ((0, 16), (16, LEVELS))
MESH = pl.DeviceIdType.MESH


def grid_of(n_col):
    return (4, 6, 2) if n_col == 48 else (2, n_col // 4, 2)


def nearest_first(z, nz):
    short = z * (nz - 1 - z) // 3
    longer = 1 - 2 * (z // (nz // 2))
    order = []
    for k in range(nz):
        both = (k + 1) // 2 * (1 if k % 2 else -1)
        two_sided = (2 * short - k + nz) // nz
        order.append(z + longer * (two_sided * both + (1 - two_sided) * (k - short)))
    return order


def copy_to(src, dst, send, recv, where):
    return pltpu.make_async_remote_copy(
        src_ref=src,
        dst_ref=dst,
        send_sem=send,
        recv_sem=recv,
        device_id=where,
        device_id_type=MESH,
    )


def wait_for(ref, sem):
    pltpu.make_async_copy(ref, ref, sem).wait()


def hand_out(result, out_h, sem):
    copy = pltpu.make_async_copy(result, out_h, sem)
    copy.start()
    copy.wait()


def kernel(
    n_tile,
    n_col,
    adj_h,
    cen_h,
    side_h,
    vert_h,
    mask_h,
    mis_h,
    cell_h,
    cnt_s,
    fp_s,
    ff_s,
    out_ref,
    adj,
    cen,
    side,
    vert,
    mask,
    cell,
    plane,
    slots,
    rows_1h,
    vals_1h,
    acc,
    y_ref,
    r_ref,
    fixed_row,
    fixed_col,
    fixed_row_in,
    fixed_col_in,
    row_out,
    row_in,
    col_out,
    col_in,
    corner_out,
    corner_in,
    fold_out,
    line_bufs,
    pick_bufs,
    group_bufs,
    top_1h,
    delta,
    delta_out,
    delta_in,
    load_sem,
    plane_send,
    plane_recv,
    slot_send,
    slot_recv,
    fixed_send,
    fixed_recv,
    halo_send,
    halo_recv,
    line_send,
    line_recv,
    pick_send,
    pick_recv,
    delta_send,
    delta_recv,
):
    nx, nz, nc = grid_of(n_col)
    ng = nx * nc
    f32 = jnp.float32
    zero = f32(0)
    me = lax.axis_index("col")
    t = lax.axis_index("tile")
    core = me % nc
    my_z = (me // nc) % nz
    my_x = me // (nc * nz)
    my_g = my_x * nc + core
    sides = ((me + 1) % n_col, (me + n_col - 1) % n_col)
    tiles = (t + 1, t - 1)
    can_go = (t < n_tile - 1, t > 0)
    can_come = (t > 0, t < n_tile - 1)
    at_top = t == n_tile - 1

    def in_plane(g):
        return (g // nc) * nc * nz + my_z * nc + g % nc

    def on_line(z):
        return my_x * nc * nz + z * nc + core

    loads = [
        pltpu.make_async_copy(src, dst, load_sem.at[i])
        for i, (src, dst) in enumerate(
            [
                (mis_h.at[my_x, :, core], plane.at[my_g]),
                (side_h, side),
                (mask_h, mask),
                (cell_h, cell),
                (adj_h, adj),
                (cen_h, cen),
                (vert_h, vert),
            ]
        )
    ]
    for load in loads:
        load.start()

    for way, outermost in ((0, t < 1), (1, t > n_tile - 2)):

        @pl.when(outermost)
        def _():
            fixed_row_in[way][...] = jnp.zeros((LEVELS, COLS), f32)
            row_in[way][...] = jnp.zeros((2, LEVELS, COLS), f32)
            for across in range(2):
                corner_in[2 * way + across][...] = jnp.zeros((8, COLS), f32)

    barrier = pltpu.get_barrier_semaphore()

    def greet(where):
        pl.semaphore_signal(barrier, inc=1, device_id=where, device_id_type=MESH)

    @pl.loop(1, nz)
    def _(i):
        greet({"col": on_line((my_z + i) % nz)})

    @pl.loop(1, ng)
    def _(i):
        greet({"col": in_plane((my_g + i) % ng)})

    for side_id in sides:
        greet({"col": side_id})
    for way in range(2):

        @pl.when(can_go[way])
        def _():
            greet({"tile": tiles[way]})
            for side_id in sides:
                greet({"tile": tiles[way], "col": side_id})

    pl.semaphore_wait(
        barrier,
        nz - 1 + ng - 1 + 2 + 3 * (jnp.where(t > 0, 1, 0) + jnp.where(t < n_tile - 1, 1, 0)),
    )

    far_way = 1 - 2 * (my_z // (nz // 2))

    @pl.loop(1, ng)
    def _(i):
        g = (my_g + i) % ng
        copy_to(
            mis_h.at[g // nc, :, g % nc],
            plane.at[my_g],
            plane_send,
            plane_recv,
            {"col": in_plane(g)},
        ).start()

    def find(s, found):
        target = fp_s[s]
        return tuple(jnp.where(target == in_plane(g), s, found[g]) for g in range(ng)) + (
            jnp.where(target == me, s, found[ng]),
        )

    sources = lax.fori_loop(0, n_col, find, (jnp.int32(0),) * (ng + 1))
    my_source = sources[ng]

    def find_again(s, found):
        target = fp_s[s]
        return tuple(jnp.where(target == sources[g], s, found[g]) for g in range(ng + 1))

    sources_2 = lax.fori_loop(0, n_col, find_again, (jnp.int32(0),) * (ng + 1))
    my_source_2 = sources_2[ng]

    lanes = lax.broadcasted_iota(jnp.int32, (LEVELS, ROWS, COLS), 2)
    rows = lax.broadcasted_iota(jnp.int32, (LEVELS, ROWS, COLS), 1)
    q_lane = lax.broadcasted_iota(jnp.int32, (VREGS, 8, COLS), 2)
    q_id = lax.broadcasted_iota(jnp.int32, (VREGS, 8, COLS), 0)
    flat_lane = lax.broadcasted_iota(jnp.int32, (LEVELS, COLS), 1)
    flat_level = lax.broadcasted_iota(jnp.int32, (LEVELS, COLS), 0)
    tile_row = lax.broadcasted_iota(jnp.int32, (8, COLS), 0)
    edge_lane = (COLS - 1, 0)
    land_lane = (0, COLS - 1)
    edge_row = (ROWS - 1, 0)
    land_row = (0, ROWS - 1)

    def pack(cube, lane):
        edge = cube.reshape(VREGS, 8, COLS)[:, :, lane : lane + 1]
        return jnp.sum(jnp.where(q_lane == q_id, edge, zero), axis=0)

    def unpack(tile):
        spread = jnp.where(q_lane == q_id, tile[None], zero)
        return jnp.sum(spread, axis=2, keepdims=True).reshape(LEVELS, ROWS, 1)

    def fold_start(n, h):
        part = 2 * n + h
        line_bufs[part][my_z] = fold_out[part][...]

        @pl.loop(1, nz)
        def _(i):
            z = (my_z + nz + far_way * (nz - i)) % nz
            copy_to(
                fold_out[part],
                line_bufs[part].at[my_z],
                line_send.at[part],
                line_recv.at[part],
                {"col": on_line(z)},
            ).start()

    def fold_wait(n, h):
        part = 2 * n + h
        wait_for(line_bufs[part].at[pl.ds(0, nz - 1)], line_recv.at[part])

    def fold_pick(n, h, chosen, to):
        part, end = 2 * n + h, 2 * to + h
        for g in range(ng):
            pick_bufs[end][g] = line_bufs[part][(chosen[g] // nc) % nz]

        @pl.loop(1, ng)
        def _(i):
            g = (my_g + i) % ng
            copy_to(
                pick_bufs[end].at[g],
                group_bufs[end].at[my_g],
                pick_send.at[end],
                pick_recv.at[end],
                {"col": in_plane(g)},
            ).start()

        group_bufs[end][my_g] = pick_bufs[end][my_g]

    def fold_finish(n, h, source, turns):
        end = 2 * n + h
        count = PARTS[h][1] - PARTS[h][0]
        wait_for(group_bufs[end].at[pl.ds(0, ng - 1)], pick_recv.at[end])
        arrived = group_bufs[end][(source // (nc * nz)) * nc + source % nc]
        backwards = COLS - 1 - lax.broadcasted_iota(jnp.int32, (count, COLS), 1)
        for column in turns:
            turned = jnp.take_along_axis(arrived, backwards, axis=1)
            arrived = jnp.where(ff_s[column] == 1, turned, arrived)
        return arrived

    loads[1].wait()
    loads[2].wait()
    ocean = mask[...].astype(f32)
    for way in range(2):
        fixed_col[way][...] = pack(side[way] * ocean, edge_lane[way])
        fixed_row[way][...] = side[2 + way, :, edge_row[way], :] * mask[
            :, edge_row[way], :
        ].astype(f32)
    fixed = [
        copy_to(
            fixed_col[way],
            fixed_col_in[way],
            fixed_send.at[way],
            fixed_recv.at[way],
            {"col": sides[way]},
        )
        for way in range(2)
    ] + [
        copy_to(
            fixed_row[way],
            fixed_row_in[way],
            fixed_send.at[2 + way],
            fixed_recv.at[2 + way],
            {"tile": tiles[way]},
        )
        for way in range(2)
    ]
    @pl.when(at_top)
    def _():
        for h, (low, high) in enumerate(PARTS):
            fold_out[4 + h][...] = fixed_row[0][low:high, :]
            fold_start(2, h)

    for way in range(2):
        fixed[way].start()
        pl.when(can_go[way])(fixed[2 + way].start)

    loads[3].wait()
    row_ids = lax.broadcasted_iota(jnp.int32, (CELL_ROWS, COLS), 0)

    def columns_of(k, g):
        return pl.ds((k * ng + g) * COLS, COLS)

    order = nearest_first(my_z, nz)
    for k in range(nz):
        for g in range(ng):
            hit = row_ids == (cell[g // nc, order[k], g % nc] >> 7)
            rows_1h[:, columns_of(k, g)] = jnp.where(hit, f32(1), zero).astype(jnp.bfloat16)

    loads[0].wait()
    wait_for(plane.at[pl.ds(0, ng - 1)], plane_recv)

    for mine in range(nz):

        @pl.when(my_z == mine)
        def _():
            for z in sorted(range(nz), key=lambda z: -abs(z - mine))[:-1]:
                k = nearest_first(z, nz).index(mine)
                copy_to(
                    plane.at[:, z],
                    slots[k],
                    slot_send.at[z],
                    slot_recv.at[k],
                    {"col": on_line(z)},
                ).start()
            slots[0][...] = plane[:, mine]

    lane_ids = lax.broadcasted_iota(jnp.int32, (COLS, COLS), 0)
    slot_ids = lax.broadcasted_iota(jnp.int32, (1, COLS), 1)

    for load in loads[4:]:
        load.wait()

    for k in range(nz):
        z, last = order[k], k == nz - 1
        if last:

            @pl.when(at_top)
            def _():
                for h in range(2):
                    fold_wait(2, h)
                    fold_pick(2, h, sources, 2)

        if k:
            wait_for(slots[k], slot_recv.at[k])

        for g in range(ng):
            count = cnt_s[(g // nc) * nc * nz + z * nc + g % nc]
            value = jnp.where(slot_ids < count, slots[k][g], zero)
            high = value.astype(jnp.bfloat16).astype(f32)
            hit = lane_ids == (cell[g // nc, z, g % nc] & 127)
            for half, part in enumerate((high, value - high)):
                vals_1h[half * COLS : (half + 1) * COLS, g * COLS : (g + 1) * COLS] = jnp.where(
                    hit, part, zero
                ).astype(jnp.bfloat16)

        def lead():
            level_ids = lax.broadcasted_iota(jnp.int32, (ROWS, COLS), 0)
            for g in range(ng):
                cell_row = cell[g // nc, z, g % nc] >> 7
                level = jnp.where((cell_row & (ROWS - 1)) == ROWS - 1, cell_row >> 5, -1)
                top_1h[:, g * COLS : (g + 1) * COLS] = jnp.where(
                    level_ids == level, f32(1), zero
                ).astype(jnp.bfloat16)
            row = lax.dot_general(
                top_1h[...],
                vals_1h[...],
                (((1,), (1,)), ((), ())),
                preferred_element_type=f32,
            )[:LEVELS]
            row = row + acc[...].reshape(LEVELS, ROWS, 2 * COLS)[:, ROWS - 1, :]
            row = adj[:, ROWS - 1, :] + row[:, :COLS] + row[:, COLS:]
            for h, (low, high) in enumerate(PARTS):
                fold_out[h][...] = side[2, low:high, ROWS - 1, :] * row[low:high]
                fold_start(0, h)

        if last:
            pl.when(at_top)(lead)
        width = ng * COLS
        term = lax.dot_general(
            rows_1h[:, k * width : (k + 1) * width],
            vals_1h[...],
            (((1,), (1,)), ((), ())),
            preferred_element_type=f32,
        )
        if k:
            acc[...] += term
        else:
            acc[...] = term

    y_ref[...] = adj[...] + (acc[:, :COLS] + acc[:, COLS:]).reshape(LEVELS, ROWS, COLS)

    def interior(y):
        to_east = side[0] * y
        to_west = side[1] * y
        north = side[2] * y
        south = side[3] * y
        up = vert[0] * y
        down = vert[1] * y
        level = jnp.zeros((1, ROWS, COLS), f32)
        r = (
            cen[...] * y
            + jnp.where(lanes == 0, zero, pltpu.roll(to_east, 1, 2))
            + jnp.where(lanes == COLS - 1, zero, pltpu.roll(to_west, COLS - 1, 2))
            + jnp.where(rows == 0, zero, pltpu.roll(north, 1, 1))
            + jnp.where(rows == ROWS - 1, zero, pltpu.roll(south, ROWS - 1, 1))
            + jnp.concatenate([up[1:], level], axis=0)
            + jnp.concatenate([level, down[:-1]], axis=0)
        )
        return r

    r_ref[...] = interior(y_ref[...])
    for way in range(2):
        col_out[way][0] = pack(side[way] * y_ref[...], edge_lane[way])
        col_out[way][1] = fixed_col[way][...] * pack(r_ref[...], edge_lane[way])
        at = edge_row[way]
        row_out[way][0] = side[2 + way, :, at, :] * y_ref[:, at, :]
        row_out[way][1] = fixed_row[way][...] * r_ref[:, at, :]
        for across in range(2):
            lane = edge_lane[across]
            spot = flat_lane == 4 * flat_level + 3 * way
            level_value = y_ref[:, at, :][:, lane : lane + 1]
            for part, weight in enumerate((side[2 + way, :, at, :], side[across, :, at, :])):
                term = weight[:, lane : lane + 1] * level_value
                corner_out[2 * way + across][part : part + 1, :] = jnp.sum(
                    jnp.where(spot, term, zero), axis=0, keepdims=True
                )

    halos = []
    for way in range(2):
        halos.append(
            copy_to(
                col_out[way],
                col_in[way],
                halo_send.at[way],
                halo_recv.at[way],
                {"col": sides[way]},
            )
        )
        halos[-1].start()
    far = []
    for way in range(2):
        far.append(
            [
                copy_to(
                    row_out[way],
                    row_in[way],
                    halo_send.at[2 + way],
                    halo_recv.at[2 + way],
                    {"tile": tiles[way]},
                )
            ]
            + [
                copy_to(
                    corner_out[2 * way + across],
                    corner_in[2 * way + across],
                    halo_send.at[4 + 2 * way + across],
                    halo_recv.at[4 + 2 * way + across],
                    {"tile": tiles[way], "col": sides[across]},
                )
                for across in range(2)
            ]
        )

        @pl.when(can_go[way])
        def _():
            for copy in far[way]:
                copy.start()

    for way in range(2):
        halos[way].wait_recv()
        fixed[way].wait_recv()

        @pl.when(can_come[way])
        def _():
            fixed[2 + way].wait_recv()
            for copy in far[way]:
                copy.wait_recv()

    def with_sides(r, west, east):
        return r + jnp.where(lanes == 0, west, jnp.where(lanes == COLS - 1, east, zero))

    for way in range(2):
        at = land_row[way]
        r_ref[:, at, :] = r_ref[:, at, :] + row_in[way][0]
    y_ref[...] = with_sides(r_ref[...], unpack(col_in[0][0]), unpack(col_in[1][0])) * mask[
        ...
    ].astype(f32)

    top = ROWS - 1
    moves = [
        copy_to(
            delta_out[way],
            delta_in[way],
            delta_send.at[way],
            delta_recv.at[way],
            {"col": sides[way]},
        )
        for way in range(2)
    ]

    @pl.when(at_top)
    def _():
        for h, (low, high) in enumerate(PARTS):
            fold_out[2 + h][...] = side[2, low:high, top, :] * y_ref[low:high, top, :]
            fold_start(1, h)
        for h in range(2):
            fold_wait(0, h)
            fold_pick(0, h, sources, 0)
        for h in range(2):
            fold_pick(0, h, sources_2, 3)
        for h, (low, high) in enumerate(PARTS):
            delta[low:high, :] = mask[low:high, top, :].astype(f32) * fold_finish(
                0, h, my_source, [my_source]
            )
        for way in range(2):
            delta_out[way][...] = side[way, :, top, :] * delta[...]
            moves[way].start()

    ring = []
    for across in range(2):
        lacked = col_out[1 - across][0]
        for way, sub in ((0, 0), (1, 7)):
            lacked = lacked + jnp.where(tile_row == sub, corner_in[2 * way + across][0:1, :], zero)
        ring.append(col_in[across][1] + fixed_col_in[across][...] * lacked)
    r_ref[...] = with_sides(interior(y_ref[...]), unpack(ring[0]), unpack(ring[1]))
    for way in range(2):
        lacked = row_out[1 - way][0]
        for across in range(2):
            spot = flat_lane == 4 * flat_level + 3 * way
            term = jnp.sum(
                jnp.where(spot, corner_in[2 * way + across][1:2, :], zero), axis=1, keepdims=True
            )
            lacked = lacked + jnp.where(flat_lane == land_lane[across], term, zero)
        at = land_row[way]
        r_ref[:, at, :] = r_ref[:, at, :] + (row_in[way][1] + fixed_row_in[way][...] * lacked)
    out_ref[...] = r_ref[...] * mask[...].astype(f32)

    @pl.when(at_top)
    def _():
        level = jnp.zeros((1, COLS), f32)
        up = vert[0, :, top, :] * delta[...]
        down = vert[1, :, top, :] * delta[...]
        change = (
            cen[:, top, :] * delta[...]
            + jnp.concatenate([up[1:], level], axis=0)
            + jnp.concatenate([level, down[:-1]], axis=0)
        )
        for way in range(2):
            moves[way].wait_recv()
            shift = 1 if way == 0 else COLS - 1
            change = change + jnp.where(
                flat_lane == land_lane[way],
                pltpu.roll(delta_in[way][...], shift, 1),
                pltpu.roll(delta_out[way][...], shift, 1),
            )
        below = side[3, :, top, :] * delta[...]
        out_ref[:, top - 1, :] = out_ref[:, top - 1, :] + below * mask[:, top - 1, :].astype(f32)
        delta[...] = change
        for h, (low, high) in enumerate(PARTS):
            delta[low:high, :] = delta[low:high, :] + fold_finish(
                2, h, my_source, [my_source]
            ) * fold_finish(3, h, my_source_2, [my_source_2, my_source])
        for h in range(2):
            fold_wait(1, h)
            fold_pick(1, h, sources, 1)
        for h, (low, high) in enumerate(PARTS):
            total = delta[low:high, :] + fold_finish(1, h, my_source, [my_source])
            out_ref[low:high, top, :] = out_ref[low:high, top, :] + total * mask[
                low:high, top, :
            ].astype(f32)
        for way in range(2):
            moves[way].wait_send()
        for part in range(6):
            wait_for(line_bufs[part].at[pl.ds(0, nz - 1)], line_send.at[part])
        for part in range(8):
            wait_for(group_bufs[part].at[pl.ds(0, ng - 1)], pick_send.at[part])

    wait_for(plane.at[pl.ds(0, ng - 1)], plane_send)

    @pl.loop(1, nz)
    def _(i):
        wait_for(slots[0], slot_send.at[(my_z + i) % nz])

    for way in range(2):
        halos[way].wait_send()
        fixed[way].wait_send()

        @pl.when(can_go[way])
        def _():
            fixed[2 + way].wait_send()
            for copy in far[way]:
                copy.wait_send()


def solution(mesh):
    n_tile, n_col = mesh.shape["tile"], mesh.shape["col"]
    nx, nz, nc = grid_of(n_col)
    ng = nx * nc
    cube = (LEVELS, ROWS, COLS)
    flat = (LEVELS, COLS)
    parts = [(high - low, COLS) for low, high in PARTS]
    f32 = jnp.float32
    any_space = pl.BlockSpec(memory_space=pl.ANY)
    scalars = pl.BlockSpec(memory_space=pltpu.SMEM)
    dma = pltpu.SemaphoreType.DMA

    def body(adj, cen, side, vert, mask, misfit, cell, count, partner, flip):
        result = pl.pallas_call(
            functools.partial(kernel, n_tile, n_col),
            out_shape=pltpu.VMEM(cube, f32),
            in_specs=[any_space] * 7 + [scalars] * 3,
            out_specs=pl.BlockSpec(memory_space=pltpu.VMEM),
            scratch_shapes=[
                pltpu.VMEM(cube, f32),
                pltpu.VMEM(cube, f32),
                pltpu.VMEM((4,) + cube, f32),
                pltpu.VMEM((2,) + cube, f32),
                pltpu.VMEM(cube, jnp.int32),
                pltpu.VMEM((nx, nz, nc, 1, COLS), jnp.int32),
                pltpu.VMEM((ng, nz, 1, COLS), f32),
                [pltpu.VMEM((ng, 1, COLS), f32)] * nz,
                pltpu.VMEM((CELL_ROWS, n_col * COLS), jnp.bfloat16),
                pltpu.VMEM((2 * COLS, ng * COLS), jnp.bfloat16),
                pltpu.VMEM((CELL_ROWS, 2 * COLS), f32),
                pltpu.VMEM(cube, f32),
                pltpu.VMEM(cube, f32),
                [pltpu.VMEM(flat, f32)] * 2,
                [pltpu.VMEM((8, COLS), f32)] * 2,
                [pltpu.VMEM(flat, f32)] * 2,
                [pltpu.VMEM((8, COLS), f32)] * 2,
                [pltpu.VMEM((2,) + flat, f32)] * 2,
                [pltpu.VMEM((2,) + flat, f32)] * 2,
                [pltpu.VMEM((2, 8, COLS), f32)] * 2,
                [pltpu.VMEM((2, 8, COLS), f32)] * 2,
                [pltpu.VMEM((8, COLS), f32)] * 4,
                [pltpu.VMEM((8, COLS), f32)] * 4,
                [pltpu.VMEM(part, f32) for part in parts * 3],
                [pltpu.VMEM((nz,) + part, f32) for part in parts * 3],
                [pltpu.VMEM((ng,) + part, f32) for part in parts * 4],
                [pltpu.VMEM((ng,) + part, f32) for part in parts * 4],
                pltpu.VMEM((ROWS, ng * COLS), jnp.bfloat16),
                pltpu.VMEM(flat, f32),
                [pltpu.VMEM(flat, f32)] * 2,
                [pltpu.VMEM(flat, f32)] * 2,
                dma((7,)),
                dma,
                dma,
                dma((nz,)),
                dma((nz,)),
                dma((4,)),
                dma((4,)),
                dma((8,)),
                dma((8,)),
                dma((6,)),
                dma((6,)),
                dma((8,)),
                dma((8,)),
                dma((2,)),
                dma((2,)),
            ],
            compiler_params=pltpu.CompilerParams(
                collective_id=0, has_side_effects=True, vmem_limit_bytes=60 * 2**20
            ),
        )(
            adj,
            cen,
            side,
            vert,
            mask,
            misfit.reshape(nx, nz, nc, 1, COLS),
            cell.reshape(nx, nz, nc, 1, COLS),
            count.reshape(n_col),
            partner,
            flip,
        )
        return pl.pallas_call(
            hand_out,
            out_shape=jax.ShapeDtypeStruct(cube, f32),
            in_specs=[pl.BlockSpec(memory_space=pltpu.VMEM)],
            out_specs=any_space,
            scratch_shapes=[dma],
            compiler_params=pltpu.CompilerParams(vmem_limit_bytes=2**20),
        )(result)

    in_specs = (
        P(None, "tile", "col"),
        P(None, "tile", "col"),
        P(None, None, "tile", "col"),
        P(None, None, "tile", "col"),
        P(None, "tile", "col"),
        P("tile", "col", None, None),
        P("tile", "col", None, None),
        P("tile", "col", None),
        P(),
        P(),
    )
    out_specs = P(None, "tile", "col")
    return jax.shard_map(body, mesh=mesh, in_specs=in_specs, out_specs=out_specs, check_vma=False)
```

```python
import functools

import jax
import jax.numpy as jnp
from jax import lax
from jax.experimental import pallas as pl
from jax.experimental.pallas import tpu as pltpu
from jax.sharding import PartitionSpec as P

LEVELS = 25
ROWS = 32
COLS = 128
CELL_ROWS = LEVELS * ROWS
VREGS = CELL_ROWS // 8
PARTS = ((0, 16), (16, LEVELS))
MESH = pl.DeviceIdType.MESH


def grid_of(n_col):
    return (4, 6, 2) if n_col == 48 else (2, n_col // 4, 2)


def nearest_first(z, nz):
    short = z * (nz - 1 - z) // 3
    longer = 1 - 2 * (z // (nz // 2))
    order = []
    for k in range(nz):
        both = (k + 1) // 2 * (1 if k % 2 else -1)
        two_sided = (2 * short - k + nz) // nz
        order.append(z + longer * (two_sided * both + (1 - two_sided) * (k - short)))
    return order


def copy_to(src, dst, send, recv, where):
    return pltpu.make_async_remote_copy(
        src_ref=src,
        dst_ref=dst,
        send_sem=send,
        recv_sem=recv,
        device_id=where,
        device_id_type=MESH,
    )


def wait_for(ref, sem):
    pltpu.make_async_copy(ref, ref, sem).wait()


def hand_out(result, out_h, sem):
    copy = pltpu.make_async_copy(result, out_h, sem)
    copy.start()
    copy.wait()


def kernel(
    n_tile,
    n_col,
    adj_h,
    cen_h,
    side_h,
    vert_h,
    mask_h,
    mis_h,
    cell_h,
    cnt_s,
    fp_s,
    ff_s,
    out_ref,
    adj,
    cen,
    side,
    vert,
    mask,
    cell,
    plane,
    slots,
    rows_1h,
    vals_1h,
    acc,
    y_ref,
    r_ref,
    fixed_row,
    fixed_col,
    fixed_row_in,
    fixed_col_in,
    row_out,
    row_in,
    col_out,
    col_in,
    corner_out,
    corner_in,
    fold_out,
    line_bufs,
    pick_bufs,
    group_bufs,
    top_1h,
    delta,
    delta_out,
    delta_in,
    load_sem,
    plane_send,
    plane_recv,
    slot_send,
    slot_recv,
    fixed_send,
    fixed_recv,
    halo_send,
    halo_recv,
    line_send,
    line_recv,
    pick_send,
    pick_recv,
    delta_send,
    delta_recv,
):
    nx, nz, nc = grid_of(n_col)
    ng = nx * nc
    f32 = jnp.float32
    zero = f32(0)
    me = lax.axis_index("col")
    t = lax.axis_index("tile")
    core = me % nc
    my_z = (me // nc) % nz
    my_x = me // (nc * nz)
    my_g = my_x * nc + core
    sides = ((me + 1) % n_col, (me + n_col - 1) % n_col)
    tiles = (t + 1, t - 1)
    can_go = (t < n_tile - 1, t > 0)
    can_come = (t > 0, t < n_tile - 1)
    at_top = t == n_tile - 1

    def in_plane(g):
        return (g // nc) * nc * nz + my_z * nc + g % nc

    def on_line(z):
        return my_x * nc * nz + z * nc + core

    loads = [
        pltpu.make_async_copy(src, dst, load_sem.at[i])
        for i, (src, dst) in enumerate(
            [
                (mis_h.at[my_x, :, core], plane.at[my_g]),
                (side_h, side),
                (mask_h, mask),
                (cell_h, cell),
                (adj_h, adj),
                (cen_h, cen),
                (vert_h, vert),
            ]
        )
    ]
    for load in loads:
        load.start()

    for way, outermost in ((0, t < 1), (1, t > n_tile - 2)):

        @pl.when(outermost)
        def _():
            fixed_row_in[way][...] = jnp.zeros((LEVELS, COLS), f32)
            row_in[way][...] = jnp.zeros((2, LEVELS, COLS), f32)
            for across in range(2):
                corner_in[2 * way + across][...] = jnp.zeros((8, COLS), f32)

    barrier = pltpu.get_barrier_semaphore()

    def greet(where):
        pl.semaphore_signal(barrier, inc=1, device_id=where, device_id_type=MESH)

    @pl.loop(1, nz)
    def _(i):
        greet({"col": on_line((my_z + i) % nz)})

    @pl.loop(1, ng)
    def _(i):
        greet({"col": in_plane((my_g + i) % ng)})

    for side_id in sides:
        greet({"col": side_id})
    for way in range(2):

        @pl.when(can_go[way])
        def _():
            greet({"tile": tiles[way]})
            for side_id in sides:
                greet({"tile": tiles[way], "col": side_id})

    pl.semaphore_wait(
        barrier,
        nz - 1 + ng - 1 + 2 + 3 * (jnp.where(t > 0, 1, 0) + jnp.where(t < n_tile - 1, 1, 0)),
    )

    far_way = 1 - 2 * (my_z // (nz // 2))

    @pl.loop(1, ng)
    def _(i):
        g = (my_g + i) % ng
        copy_to(
            mis_h.at[g // nc, :, g % nc],
            plane.at[my_g],
            plane_send,
            plane_recv,
            {"col": in_plane(g)},
        ).start()

    def find(s, found):
        target = fp_s[s]
        return tuple(jnp.where(target == in_plane(g), s, found[g]) for g in range(ng)) + (
            jnp.where(target == me, s, found[ng]),
        )

    sources = lax.fori_loop(0, n_col, find, (jnp.int32(0),) * (ng + 1))
    my_source = sources[ng]

    def find_again(s, found):
        target = fp_s[s]
        return tuple(jnp.where(target == sources[g], s, found[g]) for g in range(ng + 1))

    sources_2 = lax.fori_loop(0, n_col, find_again, (jnp.int32(0),) * (ng + 1))
    my_source_2 = sources_2[ng]

    lanes = lax.broadcasted_iota(jnp.int32, (LEVELS, ROWS, COLS), 2)
    rows = lax.broadcasted_iota(jnp.int32, (LEVELS, ROWS, COLS), 1)
    q_lane = lax.broadcasted_iota(jnp.int32, (VREGS, 8, COLS), 2)
    q_id = lax.broadcasted_iota(jnp.int32, (VREGS, 8, COLS), 0)
    flat_lane = lax.broadcasted_iota(jnp.int32, (LEVELS, COLS), 1)
    flat_level = lax.broadcasted_iota(jnp.int32, (LEVELS, COLS), 0)
    tile_row = lax.broadcasted_iota(jnp.int32, (8, COLS), 0)
    edge_lane = (COLS - 1, 0)
    land_lane = (0, COLS - 1)
    edge_row = (ROWS - 1, 0)
    land_row = (0, ROWS - 1)

    def pack(cube, lane):
        edge = cube.reshape(VREGS, 8, COLS)[:, :, lane : lane + 1]
        return jnp.sum(jnp.where(q_lane == q_id, edge, zero), axis=0)

    def unpack(tile):
        spread = jnp.where(q_lane == q_id, tile[None], zero)
        return jnp.sum(spread, axis=2, keepdims=True).reshape(LEVELS, ROWS, 1)

    def fold_start(n, h):
        part = 2 * n + h
        line_bufs[part][my_z] = fold_out[part][...]

        @pl.loop(1, nz)
        def _(i):
            z = (my_z + nz + far_way * (nz - i)) % nz
            copy_to(
                fold_out[part],
                line_bufs[part].at[my_z],
                line_send.at[part],
                line_recv.at[part],
                {"col": on_line(z)},
            ).start()

    def fold_wait(n, h):
        part = 2 * n + h
        wait_for(line_bufs[part].at[pl.ds(0, nz - 1)], line_recv.at[part])

    def fold_pick(n, h, chosen, to):
        part, end = 2 * n + h, 2 * to + h
        for g in range(ng):
            pick_bufs[end][g] = line_bufs[part][(chosen[g] // nc) % nz]

        @pl.loop(1, ng)
        def _(i):
            g = (my_g + i) % ng
            copy_to(
                pick_bufs[end].at[g],
                group_bufs[end].at[my_g],
                pick_send.at[end],
                pick_recv.at[end],
                {"col": in_plane(g)},
            ).start()

        group_bufs[end][my_g] = pick_bufs[end][my_g]

    def fold_finish(n, h, source, turns):
        end = 2 * n + h
        count = PARTS[h][1] - PARTS[h][0]
        wait_for(group_bufs[end].at[pl.ds(0, ng - 1)], pick_recv.at[end])
        arrived = group_bufs[end][(source // (nc * nz)) * nc + source % nc]
        backwards = COLS - 1 - lax.broadcasted_iota(jnp.int32, (count, COLS), 1)
        for column in turns:
            turned = jnp.take_along_axis(arrived, backwards, axis=1)
            arrived = jnp.where(ff_s[column] == 1, turned, arrived)
        return arrived

    loads[1].wait()
    loads[2].wait()
    ocean = mask[...].astype(f32)
    for way in range(2):
        fixed_col[way][...] = pack(side[way] * ocean, edge_lane[way])
        fixed_row[way][...] = side[2 + way, :, edge_row[way], :] * mask[
            :, edge_row[way], :
        ].astype(f32)
    fixed = [
        copy_to(
            fixed_col[way],
            fixed_col_in[way],
            fixed_send.at[way],
            fixed_recv.at[way],
            {"col": sides[way]},
        )
        for way in range(2)
    ] + [
        copy_to(
            fixed_row[way],
            fixed_row_in[way],
            fixed_send.at[2 + way],
            fixed_recv.at[2 + way],
            {"tile": tiles[way]},
        )
        for way in range(2)
    ]
    @pl.when(at_top)
    def _():
        for h, (low, high) in enumerate(PARTS):
            fold_out[4 + h][...] = fixed_row[0][low:high, :]
            fold_start(2, h)

    for way in range(2):
        fixed[way].start()
        pl.when(can_go[way])(fixed[2 + way].start)

    loads[3].wait()
    row_ids = lax.broadcasted_iota(jnp.int32, (CELL_ROWS, COLS), 0)

    def columns_of(k, g):
        return pl.ds((k * ng + g) * COLS, COLS)

    order = nearest_first(my_z, nz)
    for k in range(nz):
        for g in range(ng):
            hit = row_ids == (cell[g // nc, order[k], g % nc] >> 7)
            rows_1h[:, columns_of(k, g)] = jnp.where(hit, f32(1), zero).astype(jnp.bfloat16)

    loads[0].wait()
    wait_for(plane.at[pl.ds(0, ng - 1)], plane_recv)

    for mine in range(nz):

        @pl.when(my_z == mine)
        def _():
            for z in sorted(range(nz), key=lambda z: -abs(z - mine))[:-1]:
                k = nearest_first(z, nz).index(mine)
                copy_to(
                    plane.at[:, z],
                    slots[k],
                    slot_send.at[z],
                    slot_recv.at[k],
                    {"col": on_line(z)},
                ).start()
            slots[0][...] = plane[:, mine]

    lane_ids = lax.broadcasted_iota(jnp.int32, (COLS, COLS), 0)
    slot_ids = lax.broadcasted_iota(jnp.int32, (1, COLS), 1)

    for load in loads[4:]:
        load.wait()

    for k in range(nz):
        z, last = order[k], k == nz - 1
        if last:

            @pl.when(at_top)
            def _():
                for h in range(2):
                    fold_wait(2, h)
                    fold_pick(2, h, sources, 2)

        if k:
            wait_for(slots[k], slot_recv.at[k])

        for g in range(ng):
            count = cnt_s[(g // nc) * nc * nz + z * nc + g % nc]
            value = jnp.where(slot_ids < count, slots[k][g], zero)
            high = value.astype(jnp.bfloat16).astype(f32)
            hit = lane_ids == (cell[g // nc, z, g % nc] & 127)
            for half, part in enumerate((high, value - high)):
                vals_1h[half * COLS : (half + 1) * COLS, g * COLS : (g + 1) * COLS] = jnp.where(
                    hit, part, zero
                ).astype(jnp.bfloat16)

        def lead():
            level_ids = lax.broadcasted_iota(jnp.int32, (ROWS, COLS), 0)
            for g in range(ng):
                cell_row = cell[g // nc, z, g % nc] >> 7
                level = jnp.where((cell_row & (ROWS - 1)) == ROWS - 1, cell_row >> 5, -1)
                top_1h[:, g * COLS : (g + 1) * COLS] = jnp.where(
                    level_ids == level, f32(1), zero
                ).astype(jnp.bfloat16)
            row = lax.dot_general(
                top_1h[...],
                vals_1h[...],
                (((1,), (1,)), ((), ())),
                preferred_element_type=f32,
            )[:LEVELS]
            row = row + acc[...].reshape(LEVELS, ROWS, 2 * COLS)[:, ROWS - 1, :]
            row = adj[:, ROWS - 1, :] + row[:, :COLS] + row[:, COLS:]
            for h, (low, high) in enumerate(PARTS):
                fold_out[h][...] = side[2, low:high, ROWS - 1, :] * row[low:high]
                fold_start(0, h)

        if last:
            pl.when(at_top)(lead)
        width = ng * COLS
        term = lax.dot_general(
            rows_1h[:, k * width : (k + 1) * width],
            vals_1h[...],
            (((1,), (1,)), ((), ())),
            preferred_element_type=f32,
        )
        if k:
            acc[...] += term
        else:
            acc[...] = term

    y_ref[...] = adj[...] + (acc[:, :COLS] + acc[:, COLS:]).reshape(LEVELS, ROWS, COLS)

    def interior(y):
        to_east = side[0] * y
        to_west = side[1] * y
        north = side[2] * y
        south = side[3] * y
        up = vert[0] * y
        down = vert[1] * y
        level = jnp.zeros((1, ROWS, COLS), f32)
        r = (
            cen[...] * y
            + jnp.where(lanes == 0, zero, pltpu.roll(to_east, 1, 2))
            + jnp.where(lanes == COLS - 1, zero, pltpu.roll(to_west, COLS - 1, 2))
            + jnp.where(rows == 0, zero, pltpu.roll(north, 1, 1))
            + jnp.where(rows == ROWS - 1, zero, pltpu.roll(south, ROWS - 1, 1))
            + jnp.concatenate([up[1:], level], axis=0)
            + jnp.concatenate([level, down[:-1]], axis=0)
        )
        return r

    r_ref[...] = interior(y_ref[...])
    for way in range(2):
        col_out[way][0] = pack(side[way] * y_ref[...], edge_lane[way])
        col_out[way][1] = fixed_col[way][...] * pack(r_ref[...], edge_lane[way])
        at = edge_row[way]
        row_out[way][0] = side[2 + way, :, at, :] * y_ref[:, at, :]
        row_out[way][1] = fixed_row[way][...] * r_ref[:, at, :]
        for across in range(2):
            lane = edge_lane[across]
            spot = flat_lane == 4 * flat_level + 3 * way
            level_value = y_ref[:, at, :][:, lane : lane + 1]
            for part, weight in enumerate((side[2 + way, :, at, :], side[across, :, at, :])):
                term = weight[:, lane : lane + 1] * level_value
                corner_out[2 * way + across][part : part + 1, :] = jnp.sum(
                    jnp.where(spot, term, zero), axis=0, keepdims=True
                )

    halos = []
    for way in range(2):
        halos.append(
            copy_to(
                col_out[way],
                col_in[way],
                halo_send.at[way],
                halo_recv.at[way],
                {"col": sides[way]},
            )
        )
        halos[-1].start()
    far = []
    for way in range(2):
        far.append(
            [
                copy_to(
                    row_out[way],
                    row_in[way],
                    halo_send.at[2 + way],
                    halo_recv.at[2 + way],
                    {"tile": tiles[way]},
                )
            ]
            + [
                copy_to(
                    corner_out[2 * way + across],
                    corner_in[2 * way + across],
                    halo_send.at[4 + 2 * way + across],
                    halo_recv.at[4 + 2 * way + across],
                    {"tile": tiles[way], "col": sides[across]},
                )
                for across in range(2)
            ]
        )

        @pl.when(can_go[way])
        def _():
            for copy in far[way]:
                copy.start()

    @pl.when(at_top)
    def _():
        for h in range(2):
            fold_wait(0, h)
            fold_pick(0, h, sources, 0)

    for way in range(2):
        halos[way].wait_recv()
        fixed[way].wait_recv()

        @pl.when(can_come[way])
        def _():
            fixed[2 + way].wait_recv()
            for copy in far[way]:
                copy.wait_recv()

    def with_sides(r, west, east):
        return r + jnp.where(lanes == 0, west, jnp.where(lanes == COLS - 1, east, zero))

    for way in range(2):
        at = land_row[way]
        r_ref[:, at, :] = r_ref[:, at, :] + row_in[way][0]
    y_ref[...] = with_sides(r_ref[...], unpack(col_in[0][0]), unpack(col_in[1][0])) * mask[
        ...
    ].astype(f32)

    top = ROWS - 1
    moves = [
        copy_to(
            delta_out[way],
            delta_in[way],
            delta_send.at[way],
            delta_recv.at[way],
            {"col": sides[way]},
        )
        for way in range(2)
    ]

    @pl.when(at_top)
    def _():
        for h, (low, high) in enumerate(PARTS):
            fold_out[2 + h][...] = side[2, low:high, top, :] * y_ref[low:high, top, :]
            fold_start(1, h)
        for h in range(2):
            fold_pick(0, h, sources_2, 3)
        for h, (low, high) in enumerate(PARTS):
            delta[low:high, :] = mask[low:high, top, :].astype(f32) * fold_finish(
                0, h, my_source, [my_source]
            )
        for way in range(2):
            delta_out[way][...] = side[way, :, top, :] * delta[...]
            moves[way].start()

    ring = []
    for across in range(2):
        lacked = col_out[1 - across][0]
        for way, sub in ((0, 0), (1, 7)):
            lacked = lacked + jnp.where(tile_row == sub, corner_in[2 * way + across][0:1, :], zero)
        ring.append(col_in[across][1] + fixed_col_in[across][...] * lacked)
    r_ref[...] = with_sides(interior(y_ref[...]), unpack(ring[0]), unpack(ring[1]))
    for way in range(2):
        lacked = row_out[1 - way][0]
        for across in range(2):
            spot = flat_lane == 4 * flat_level + 3 * way
            term = jnp.sum(
                jnp.where(spot, corner_in[2 * way + across][1:2, :], zero), axis=1, keepdims=True
            )
            lacked = lacked + jnp.where(flat_lane == land_lane[across], term, zero)
        at = land_row[way]
        r_ref[:, at, :] = r_ref[:, at, :] + (row_in[way][1] + fixed_row_in[way][...] * lacked)
    out_ref[...] = r_ref[...] * mask[...].astype(f32)

    @pl.when(at_top)
    def _():
        level = jnp.zeros((1, COLS), f32)
        up = vert[0, :, top, :] * delta[...]
        down = vert[1, :, top, :] * delta[...]
        change = (
            cen[:, top, :] * delta[...]
            + jnp.concatenate([up[1:], level], axis=0)
            + jnp.concatenate([level, down[:-1]], axis=0)
        )
        for way in range(2):
            moves[way].wait_recv()
            shift = 1 if way == 0 else COLS - 1
            change = change + jnp.where(
                flat_lane == land_lane[way],
                pltpu.roll(delta_in[way][...], shift, 1),
                pltpu.roll(delta_out[way][...], shift, 1),
            )
        below = side[3, :, top, :] * delta[...]
        out_ref[:, top - 1, :] = out_ref[:, top - 1, :] + below * mask[:, top - 1, :].astype(f32)
        delta[...] = change
        for h, (low, high) in enumerate(PARTS):
            delta[low:high, :] = delta[low:high, :] + fold_finish(
                2, h, my_source, [my_source]
            ) * fold_finish(3, h, my_source_2, [my_source_2, my_source])
        for h in range(2):
            fold_wait(1, h)
            fold_pick(1, h, sources, 1)
        for h, (low, high) in enumerate(PARTS):
            total = delta[low:high, :] + fold_finish(1, h, my_source, [my_source])
            out_ref[low:high, top, :] = out_ref[low:high, top, :] + total * mask[
                low:high, top, :
            ].astype(f32)
        for way in range(2):
            moves[way].wait_send()
        for part in range(6):
            wait_for(line_bufs[part].at[pl.ds(0, nz - 1)], line_send.at[part])
        for part in range(8):
            wait_for(group_bufs[part].at[pl.ds(0, ng - 1)], pick_send.at[part])

    wait_for(plane.at[pl.ds(0, ng - 1)], plane_send)

    @pl.loop(1, nz)
    def _(i):
        wait_for(slots[0], slot_send.at[(my_z + i) % nz])

    for way in range(2):
        halos[way].wait_send()
        fixed[way].wait_send()

        @pl.when(can_go[way])
        def _():
            fixed[2 + way].wait_send()
            for copy in far[way]:
                copy.wait_send()


def solution(mesh):
    n_tile, n_col = mesh.shape["tile"], mesh.shape["col"]
    nx, nz, nc = grid_of(n_col)
    ng = nx * nc
    cube = (LEVELS, ROWS, COLS)
    flat = (LEVELS, COLS)
    parts = [(high - low, COLS) for low, high in PARTS]
    f32 = jnp.float32
    any_space = pl.BlockSpec(memory_space=pl.ANY)
    scalars = pl.BlockSpec(memory_space=pltpu.SMEM)
    dma = pltpu.SemaphoreType.DMA

    def body(adj, cen, side, vert, mask, misfit, cell, count, partner, flip):
        result = pl.pallas_call(
            functools.partial(kernel, n_tile, n_col),
            out_shape=pltpu.VMEM(cube, f32),
            in_specs=[any_space] * 7 + [scalars] * 3,
            out_specs=pl.BlockSpec(memory_space=pltpu.VMEM),
            scratch_shapes=[
                pltpu.VMEM(cube, f32),
                pltpu.VMEM(cube, f32),
                pltpu.VMEM((4,) + cube, f32),
                pltpu.VMEM((2,) + cube, f32),
                pltpu.VMEM(cube, jnp.int32),
                pltpu.VMEM((nx, nz, nc, 1, COLS), jnp.int32),
                pltpu.VMEM((ng, nz, 1, COLS), f32),
                [pltpu.VMEM((ng, 1, COLS), f32)] * nz,
                pltpu.VMEM((CELL_ROWS, n_col * COLS), jnp.bfloat16),
                pltpu.VMEM((2 * COLS, ng * COLS), jnp.bfloat16),
                pltpu.VMEM((CELL_ROWS, 2 * COLS), f32),
                pltpu.VMEM(cube, f32),
                pltpu.VMEM(cube, f32),
                [pltpu.VMEM(flat, f32)] * 2,
                [pltpu.VMEM((8, COLS), f32)] * 2,
                [pltpu.VMEM(flat, f32)] * 2,
                [pltpu.VMEM((8, COLS), f32)] * 2,
                [pltpu.VMEM((2,) + flat, f32)] * 2,
                [pltpu.VMEM((2,) + flat, f32)] * 2,
                [pltpu.VMEM((2, 8, COLS), f32)] * 2,
                [pltpu.VMEM((2, 8, COLS), f32)] * 2,
                [pltpu.VMEM((8, COLS), f32)] * 4,
                [pltpu.VMEM((8, COLS), f32)] * 4,
                [pltpu.VMEM(part, f32) for part in parts * 3],
                [pltpu.VMEM((nz,) + part, f32) for part in parts * 3],
                [pltpu.VMEM((ng,) + part, f32) for part in parts * 4],
                [pltpu.VMEM((ng,) + part, f32) for part in parts * 4],
                pltpu.VMEM((ROWS, ng * COLS), jnp.bfloat16),
                pltpu.VMEM(flat, f32),
                [pltpu.VMEM(flat, f32)] * 2,
                [pltpu.VMEM(flat, f32)] * 2,
                dma((7,)),
                dma,
                dma,
                dma((nz,)),
                dma((nz,)),
                dma((4,)),
                dma((4,)),
                dma((8,)),
                dma((8,)),
                dma((6,)),
                dma((6,)),
                dma((8,)),
                dma((8,)),
                dma((2,)),
                dma((2,)),
            ],
            compiler_params=pltpu.CompilerParams(
                collective_id=0, has_side_effects=True, vmem_limit_bytes=60 * 2**20
            ),
        )(
            adj,
            cen,
            side,
            vert,
            mask,
            misfit.reshape(nx, nz, nc, 1, COLS),
            cell.reshape(nx, nz, nc, 1, COLS),
            count.reshape(n_col),
            partner,
            flip,
        )
        return pl.pallas_call(
            hand_out,
            out_shape=jax.ShapeDtypeStruct(cube, f32),
            in_specs=[pl.BlockSpec(memory_space=pltpu.VMEM)],
            out_specs=any_space,
            scratch_shapes=[dma],
            compiler_params=pltpu.CompilerParams(vmem_limit_bytes=2**20),
        )(result)

    in_specs = (
        P(None, "tile", "col"),
        P(None, "tile", "col"),
        P(None, None, "tile", "col"),
        P(None, None, "tile", "col"),
        P(None, "tile", "col"),
        P("tile", "col", None, None),
        P("tile", "col", None, None),
        P("tile", "col", None),
        P(),
        P(),
    )
    out_specs = P(None, "tile", "col")
    return jax.shard_map(body, mesh=mesh, in_specs=in_specs, out_specs=out_specs, check_vma=False)
```
